32 devices in a mesh: groups: 2 (over y), context: 8 (over z, x), tensor: 2 (over core).
Axes of the slice: x: 2, y: 2, z: 4, core: 2. Of those that a mesh axis runs over, the one named last changes fastest.
Arguments:
- self_queries: bfloat16 [1280, 2048], P(('groups', 'context'), 'tensor'), parts along dimension 0, may hold values from -512 to 512
- self_keys: bfloat16 [1280, 512], P(('groups', 'context'), 'tensor'), parts along dimension 0, may hold values from -6 to 6
- self_values: bfloat16 [1280, 512], P(('groups', 'context'), 'tensor'), parts along dimension 0, may hold values from -6 to 6
- cross_queries: bfloat16 [1280, 2048], P(('groups', 'context'), 'tensor'), parts along dimension 0, may hold values from -512 to 512
- cross_keys: bfloat16 [384, 512], P(('groups', 'context'), 'tensor'), parts along dimension 0, may hold values from -6 to 6
- cross_values: bfloat16 [384, 512], P(('groups', 'context'), 'tensor'), parts along dimension 0, may hold values from -6 to 6
- span_order: int32 [32], P('groups'), parts along dimension 0, may hold values from 0 to 15, as said below
Outputs:
- self_out: bfloat16 [1280, 2048], P(('groups', 'context'), 'tensor'), parts along dimension 0
- cross_out: bfloat16 [1280, 2048], P(('groups', 'context'), 'tensor'), parts along dimension 0
The draws below stay inside these ranges and needn't reach their ends.
There are 2 independent parts, one for each index of `groups`. The reference program is written for one: setup_inputs(seed, part) draws one part's arguments, and reference() takes and returns one part's arrays. A program takes and returns all parts, laid end to end along the dimension named above; each array names one. Nothing has to cross between parts.
Inputs may be any that keep to these rules, and one draw needn't show every extreme that they name: `span_order`: each of 0 to 15 appears once, and entries 2 d and 2 d + 1 sum to 15.
All inputs are finite; a program needn't handle non-finite values.
Results may differ from the reference program's by a relative error of at most 0.012.
The reference program's roundings to bfloat16 on the way count: a program that leaves them out, or rounds other values in their place, can miss the bound.
Values may be sent and summed in bfloat16 or wider, within the bound.
A program may use at most 128 MiB of HBM per device.

```python
import jax
import jax.numpy as jnp
from jax import lax

HEAD_DIM = 128
HEADS = 16
KV_HEADS = 4
TEXT = 640
IMAGE = 192
SPAN = 40
SPANS = 16


def self_draw(key):
    key_query, key_key = jax.random.split(jax.random.fold_in(key, 17), 2)
    key_rows = jnp.clip(jax.random.normal(key_key, (TEXT, KV_HEADS, HEAD_DIM), jnp.float32), -6.0, 6.0)
    query_rows = jnp.clip(2.5 * jax.random.normal(key_query, (TEXT, HEADS, HEAD_DIM), jnp.float32), -15.0, 15.0)
    return (query_rows.reshape(TEXT, HEADS * HEAD_DIM), key_rows.reshape(TEXT, KV_HEADS * HEAD_DIM))


def cross_draw(key):
    key_query, key_key = jax.random.split(jax.random.fold_in(key, 29), 2)
    key_rows = jnp.clip(jax.random.normal(key_key, (IMAGE, KV_HEADS, HEAD_DIM), jnp.float32), -6.0, 6.0)
    query_rows = jnp.clip(2.5 * jax.random.normal(key_query, (TEXT, HEADS, HEAD_DIM), jnp.float32), -15.0, 15.0)
    return (query_rows.reshape(TEXT, HEADS * HEAD_DIM), key_rows.reshape(IMAGE, KV_HEADS * HEAD_DIM))


def draw_self_queries(key, part):
    return self_draw(key)[0].astype(jnp.bfloat16)


def draw_self_keys(key, part):
    return self_draw(key)[1].astype(jnp.bfloat16)


def draw_cross_queries(key, part):
    return cross_draw(key)[0].astype(jnp.bfloat16)


def draw_cross_keys(key, part):
    return cross_draw(key)[1].astype(jnp.bfloat16)


def draw_span_order(key, part):
    half_count = SPANS // 2
    key_owner, key_flip = jax.random.split(jax.random.fold_in(key, 5))
    owner = jax.random.permutation(key_owner, half_count).astype(jnp.int32)
    flipped = jax.random.randint(key_flip, (half_count,), 0, 2)
    late_span = SPANS - 1 - owner
    first_span = jnp.where(flipped == 1, late_span, owner)
    second_span = jnp.where(flipped == 1, owner, late_span)
    return jnp.stack([first_span, second_span], 1).reshape(-1).astype(jnp.int32)


def block_levels(own_key, dims, cuts, low, top_value):
    level = 1.0
    for position, shards_of in cuts:
        heights = jax.random.uniform(jax.random.fold_in(jax.random.fold_in(own_key, 6), position), (shards_of,), jnp.float32, low / len(cuts), top_value / len(cuts))
        level = level * jnp.repeat(jnp.exp(heights), dims[position] // shards_of).reshape((-1,) + (1,) * (len(dims) - 1 - position))
    return level


def noise(key, dims, scale, most, cuts=(), kind=jnp.bfloat16):
    array = scale * jax.random.normal(key, dims, jnp.float32)
    if cuts:
        array = array * block_levels(key, dims, cuts, -0.22, 0.18)
    return jnp.clip(array, -most, most).astype(kind)


def setup_inputs(seed: int = 0, part: int = 0) -> dict:
    arg_keys = jax.random.split(jax.random.key(seed), 8)
    own_keys = jax.random.split(jax.random.fold_in(arg_keys[7], part), 8)
    self_queries = draw_self_queries(jax.random.fold_in(jax.random.fold_in(arg_keys[7], part), 71), part)
    self_keys = draw_self_keys(jax.random.fold_in(jax.random.fold_in(arg_keys[7], part), 71), part)
    self_values = noise(own_keys[2], (TEXT, KV_HEADS * HEAD_DIM), 1.0, 6.0, ((0, 8), (1, 2)))
    cross_queries = draw_cross_queries(jax.random.fold_in(jax.random.fold_in(arg_keys[7], part), 71), part)
    cross_keys = draw_cross_keys(jax.random.fold_in(jax.random.fold_in(arg_keys[7], part), 71), part)
    cross_values = noise(own_keys[5], (IMAGE, KV_HEADS * HEAD_DIM), 1.0, 6.0, ((0, 8), (1, 2)))
    span_order = draw_span_order(jax.random.fold_in(jax.random.fold_in(arg_keys[7], part), 71), part)
    return {"self_queries": self_queries, "self_keys": self_keys, "self_values": self_values, "cross_queries": cross_queries, "cross_keys": cross_keys, "cross_values": cross_values, "span_order": span_order}


def rotary(values, places):
    half_dim = values.shape[-1] // 2
    frequency = 500000.0 ** (-(jnp.arange(half_dim, dtype=jnp.float32) * 2.0) / values.shape[-1])
    angles = places.astype(jnp.float32)[:, None] * frequency[None, :]
    cosine = jnp.cos(angles)[:, None, :]
    sine_part = jnp.sin(angles)[:, None, :]
    first_half = values[..., :half_dim]
    second_half = values[..., half_dim:]
    return jnp.concatenate([first_half * cosine - second_half * sine_part, second_half * cosine + first_half * sine_part], -1)


def attend_block(queries, key_rows, value_rows, query_places, key_places):
    scores = jnp.einsum("qkgd,rkd->kgqr", queries.astype(jnp.float32), key_rows.astype(jnp.float32)) * (HEAD_DIM ** -0.5)
    if key_places is not None:
        allowed = key_places[None, :] <= query_places[:, None]
        scores = jnp.where(allowed[None, None], scores, -jnp.inf)
    row_peak = jnp.max(scores, -1, keepdims=True)
    weights = jnp.exp(scores - row_peak)
    weight_sum = jnp.sum(weights, -1)
    rounded = lax.optimization_barrier(weights.astype(jnp.bfloat16))
    mixed_sum = jnp.einsum("kgqr,rkd->qkgd", rounded.astype(jnp.float32), value_rows.astype(jnp.float32))
    return mixed_sum / jnp.transpose(weight_sum, (2, 0, 1))[..., None]


def attention(queries, key_rows, value_rows, query_places, key_places):
    row_total = queries.shape[0]
    block_rows = min(512, row_total)
    while row_total % block_rows != 0:
        block_rows = block_rows // 2
    query_blocks = queries.reshape((row_total // block_rows, block_rows) + queries.shape[1:])
    if key_places is None:
        def per_block(query_block):
            return attend_block(query_block, key_rows, value_rows, None, None)
        result = lax.map(per_block, query_blocks)
    else:
        place_blocks = query_places.reshape(row_total // block_rows, block_rows)

        def per_masked(arrived):
            return attend_block(arrived[0], key_rows, value_rows, arrived[1], key_places)
        result = lax.map(per_masked, (query_blocks, place_blocks))
    return result.reshape(row_total, -1).astype(jnp.bfloat16)


def reference(self_queries, self_keys, self_values, cross_queries, cross_keys, cross_values, span_order):
    group_size = HEADS // KV_HEADS
    places = (span_order[:, None] * SPAN + jnp.arange(SPAN, dtype=jnp.int32)[None, :]).reshape(-1).astype(jnp.int32)
    text_queries = rotary(self_queries.astype(jnp.float32).reshape(TEXT, HEADS, HEAD_DIM), places).astype(jnp.bfloat16)
    text_queries = lax.optimization_barrier(text_queries).reshape(TEXT, KV_HEADS, group_size, HEAD_DIM)
    text_keys = rotary(self_keys.astype(jnp.float32).reshape(TEXT, KV_HEADS, HEAD_DIM), places).astype(jnp.bfloat16)
    text_keys = lax.optimization_barrier(text_keys)
    self_out = attention(text_queries, text_keys, self_values.reshape(TEXT, KV_HEADS, HEAD_DIM), places, places)
    image_queries = cross_queries.reshape(TEXT, KV_HEADS, group_size, HEAD_DIM)
    cross_out = attention(image_queries, cross_keys.reshape(IMAGE, KV_HEADS, HEAD_DIM), cross_values.reshape(IMAGE, KV_HEADS, HEAD_DIM), None, None)
    return (self_out, cross_out)
```

```python
import functools
import math

import jax
import jax.numpy as jnp
import numpy as np
from jax import lax
from jax.experimental import pallas as pl
from jax.experimental.pallas import tpu as pltpu
from jax.sharding import PartitionSpec as P

HEAD_DIM = 128
HEADS = 16
KV_HEADS = 4
GROUP = HEADS // KV_HEADS
NEG_FILL = -1e30
SCALE = HEAD_DIM ** (-0.5) * math.log2(math.e)


def rotary_tables(spans, span_len):
    half = HEAD_DIM // 2
    frequency = 500000.0 ** (-(np.arange(half) * 2.0) / HEAD_DIM)
    frequency = np.concatenate([frequency, frequency])
    base = (np.arange(spans) * span_len)[:, None] * frequency[None, :]
    inner = np.arange(span_len)[:, None] * frequency[None, :]
    sign = np.where(np.arange(HEAD_DIM) < half, -1.0, 1.0)[None, :]
    inners = [np.cos(inner), np.sin(inner), np.cos(inner) * sign, np.sin(inner) * sign]
    return np.concatenate(inners + [np.cos(base), np.sin(base)]).astype(np.float32)


def doubling(order):
    held, steps = [0], []
    for mask in order:
        steps.append((mask, list(held)))
        held += [item ^ mask for item in held]
    return steps


def kernel(
    n, nx,
    order_hbm, q_hbm, k_hbm, v_hbm, cq_hbm, ck_hbm, cv_hbm, tables_hbm,
    out_v, cout_v,
    text, image, qs, tables, q_rot, peak, total, mixed, order,
    load_sem, send_sem, text_recv, image_recv,
):
    me = lax.axis_index("context")
    rows = qs.shape[1]
    span_len = rows // 2
    kv_local = text.shape[3] // HEAD_DIM
    image_rows = image.shape[2]

    x_masks = [1 << b for b in reversed(range(nx.bit_length() - 1))]
    z_masks = [nx << b for b in reversed(range((n // nx).bit_length() - 1))]
    masks = z_masks + x_masks
    z_x = doubling(z_masks + x_masks)
    z_x_z = doubling(z_masks[:1] + x_masks + z_masks[1:])
    x_z = doubling(x_masks + z_masks)
    part_steps = (z_x, z_x)
    image_steps = x_z

    def flipped(index, item):
        for mask in masks:
            bit = (item // mask) % 2
            index = index + mask * bit * (1 - 2 * ((index // mask) % 2))
        return index

    partner = {mask: flipped(me, mask) for mask in masks}

    barrier = pltpu.get_barrier_semaphore()
    for mask in masks:
        pl.semaphore_signal(
            barrier, inc=1, device_id={"context": partner[mask]},
            device_id_type=pl.DeviceIdType.MESH)
    kv_loads = [
        pltpu.make_async_copy(k_hbm, text.at[0, 0], load_sem.at[0]),
        pltpu.make_async_copy(v_hbm, text.at[0, 1], load_sem.at[0]),
        pltpu.make_async_copy(ck_hbm, image.at[0, 0], load_sem.at[1]),
        pltpu.make_async_copy(cv_hbm, image.at[0, 1], load_sem.at[1]),
    ]
    other_loads = [
        pltpu.make_async_copy(order_hbm, order, load_sem.at[2]),
        pltpu.make_async_copy(tables_hbm, tables, load_sem.at[3]),
        pltpu.make_async_copy(q_hbm, qs.at[0], load_sem.at[4]),
        pltpu.make_async_copy(cq_hbm, qs.at[1], load_sem.at[4]),
    ]

    def landed(ref, sem):
        pltpu.make_async_copy(ref, ref, sem).wait()

    for load in kv_loads:
        load.start()
    for load in other_loads:
        load.start()
    landed(text.at[0], load_sem.at[0])
    landed(image.at[0], load_sem.at[1])
    pl.semaphore_wait(barrier, len(masks))

    def text_copy(item, part, mask):
        return pltpu.make_async_remote_copy(
            src_ref=text.at[item, part], dst_ref=text.at[item ^ mask, part],
            send_sem=send_sem.at[0], recv_sem=text_recv.at[(item ^ mask) - 1, part],
            device_id={"context": partner[mask]}, device_id_type=pl.DeviceIdType.MESH)

    def image_copy(item, mask):
        return pltpu.make_async_remote_copy(
            src_ref=image.at[item], dst_ref=image.at[item ^ mask],
            send_sem=send_sem.at[1], recv_sem=image_recv.at[(item ^ mask) - 1],
            device_id={"context": partner[mask]}, device_id_type=pl.DeviceIdType.MESH)

    def forward_text(item, part):
        for mask, held in part_steps[part]:
            if item in held:
                text_copy(item, part, mask).start()

    def forward_image(item):
        for mask, held in image_steps:
            if item in held:
                image_copy(item, mask).start()

    def arrive_text(item, part):
        text_copy(item ^ masks[0], part, masks[0]).wait_recv()
        forward_text(item, part)

    def arrive_image(item):
        image_copy(item ^ masks[0], masks[0]).wait_recv()
        forward_image(item)

    forward_text(0, 0)
    forward_text(0, 1)
    forward_image(0)

    other_loads[0].wait()
    other_loads[1].wait()
    landed(qs, load_sem.at[4])

    spans = order.shape[0]

    def angles(place):
        inners = [tables[at * span_len:(at + 1) * span_len, :] for at in range(4)]
        cosines, sines, starts = [], [], []
        for part in range(2):
            span = order[2 * place + part]
            base_cos = tables[pl.ds(4 * span_len + span, 1), :]
            base_sin = tables[pl.ds(4 * span_len + spans + span, 1), :]
            cosines.append(base_cos * inners[0] - base_sin * inners[1])
            sines.append(base_sin * inners[2] + base_cos * inners[3])
            starts.append(span * span_len)
        return jnp.concatenate(cosines, 0), jnp.concatenate(sines, 0), starts

    def rotate(values, cosine, sine):
        values = values.astype(jnp.float32)
        turned = pltpu.roll(values, HEAD_DIM // 2, 1)
        return (values * cosine + turned * sine).astype(jnp.bfloat16)

    def positions(starts, shape, axis):
        index = lax.broadcasted_iota(jnp.int32, shape, axis)
        result = starts[0] + index
        for at in range(1, len(starts)):
            result = jnp.where(index < at * span_len, result, starts[at] + index - at * span_len)
        return result

    own_cos, own_sin, own_starts = angles(me)
    own_places = positions(own_starts, (rows, 1), 0)
    for head in range(kv_local * GROUP):
        q_rot[head // GROUP, pl.ds(head % GROUP * rows, rows), :] = rotate(
            qs[0, :, head * HEAD_DIM:(head + 1) * HEAD_DIM], own_cos, own_sin)

    def dot_nt(a, b):
        return lax.dot_general(a, b, (((1,), (1,)), ((), ())), preferred_element_type=jnp.float32)

    def join(pieces):
        return pieces[0] if len(pieces) == 1 else jnp.concatenate(pieces, 0)

    def block(items, first=False, last=False):
        parts = [angles(flipped(me, item)) for item in items]
        cosine, sine = join([p[0] for p in parts]), join([p[1] for p in parts])
        width = rows * len(items)
        allowed = positions(sum([p[2] for p in parts], []), (1, width), 1) <= own_places
        for head in range(kv_local):
            columns = slice(head * HEAD_DIM, (head + 1) * HEAD_DIM)
            keys = rotate(join([text[item, 0, :, columns] for item in items]), cosine, sine)
            scores = dot_nt(q_rot[head], keys) * SCALE
            scores = jnp.where(allowed[None], scores.reshape(GROUP, rows, width), NEG_FILL)
            scores = scores.reshape(GROUP * rows, width)
            top = jnp.max(scores, -1, keepdims=True)
            if not first:
                old = peak[head]
                top = jnp.maximum(top, old)
            weights = jnp.exp2(scores - top)
            summed = jnp.sum(weights, -1, keepdims=True)
            product = jnp.dot(
                weights.astype(jnp.bfloat16), join([text[item, 1, :, columns] for item in items]),
                preferred_element_type=jnp.float32)
            if not first:
                factor = jnp.exp2(old - top)
                summed = summed + total[head] * factor
                product = product + mixed[head] * factor
            if last:
                store(out_v, head, product / summed)
            else:
                peak[head] = top
                total[head] = summed
                mixed[head] = product

    def store(target, head, result):
        result = result.astype(jnp.bfloat16)
        for g in range(GROUP):
            at = head * GROUP + g
            target[:, at * HEAD_DIM:(at + 1) * HEAD_DIM] = result[g * rows:(g + 1) * rows]

    def cross():
        keys_all = image[:, 0].astype(jnp.float32).reshape(n * image_rows, -1).astype(jnp.bfloat16)
        values_all = image[:, 1].astype(jnp.float32).reshape(n * image_rows, -1).astype(jnp.bfloat16)
        for head in range(kv_local):
            columns = slice(head * HEAD_DIM, (head + 1) * HEAD_DIM)
            queries = jnp.concatenate(
                [qs[1, :, h * HEAD_DIM:(h + 1) * HEAD_DIM] for h in range(head * GROUP, (head + 1) * GROUP)], 0)
            scores = dot_nt(queries, keys_all[:, columns]) * SCALE
            weights = jnp.exp2(scores - jnp.max(scores, -1, keepdims=True))
            summed = jnp.sum(weights, -1, keepdims=True)
            product = jnp.dot(
                weights.astype(jnp.bfloat16), values_all[:, columns], preferred_element_type=jnp.float32)
            store(cout_v, head, product / summed)

    def run_events(events):
        for event in events:
            kind, items = event[0], [int(digit) for digit in event[1:]]
            if kind == "B":
                block(items)
            elif kind == "L":
                block(items, last=True)
            elif kind == "C":
                cross()
            elif kind == "i":
                for item in items:
                    arrive_image(item)
            else:
                for item in items:
                    arrive_text(item, "KV".index(kind))

    block([0], first=True)
    if n == 8 and nx == 2:
        run_events((
            "K4", "V4", "K2", "V2", "K1", "V1", "i1", "i4", "B124", "K6", "V6", "i5",
            "K3", "V3", "K5", "V5", "B356", "i2367", "C", "K7", "V7", "L7"))
    else:
        for part in range(2):
            for mask, held in part_steps[part]:
                for item in held:
                    arrive_text(item ^ mask, part)
        for mask, held in image_steps:
            for item in held:
                arrive_image(item ^ mask)

        def step(item, unused):
            block([item])
            return 0

        lax.fori_loop(1, n, step, 0)
        for head in range(kv_local):
            store(out_v, head, mixed[head] / total[head])
        cross()
    landed(text.at[pl.ds(0, n - 1)], send_sem.at[0])
    landed(image.at[pl.ds(0, n - 1)], send_sem.at[1])


def flush(self_v, cross_v, self_hbm, cross_hbm, sems):
    copies = [
        pltpu.make_async_copy(self_v, self_hbm, sems.at[0]),
        pltpu.make_async_copy(cross_v, cross_hbm, sems.at[1]),
    ]
    for copy in copies:
        copy.start()
    for copy in copies:
        copy.wait()


def body(n, nx, self_queries, self_keys, self_values, cross_queries, cross_keys, cross_values, span_order):
    rows, width = self_queries.shape
    kv_width = self_keys.shape[1]
    kv_local = kv_width // HEAD_DIM
    image_rows = cross_keys.shape[0]
    tables = rotary_tables(span_order.shape[0], rows // 2)
    anywhere = pl.BlockSpec(memory_space=pl.ANY)
    result = pltpu.VMEM((rows, width), jnp.bfloat16)
    held = pl.pallas_call(
        functools.partial(kernel, n, nx),
        out_shape=(result, result),
        in_specs=[anywhere] * 8,
        out_specs=(pl.BlockSpec(memory_space=pltpu.VMEM),) * 2,
        scratch_shapes=[
            pltpu.VMEM((n, 2, rows, kv_width), jnp.bfloat16),
            pltpu.VMEM((n, 2, image_rows, kv_width), jnp.bfloat16),
            pltpu.VMEM((2, rows, width), jnp.bfloat16),
            pltpu.VMEM(tables.shape, jnp.float32),
            pltpu.VMEM((kv_local, GROUP * rows, HEAD_DIM), jnp.bfloat16),
            pltpu.VMEM((kv_local, GROUP * rows, 1), jnp.float32),
            pltpu.VMEM((kv_local, GROUP * rows, 1), jnp.float32),
            pltpu.VMEM((kv_local, GROUP * rows, HEAD_DIM), jnp.float32),
            pltpu.SMEM(span_order.shape, jnp.int32),
            pltpu.SemaphoreType.DMA((5,)),
            pltpu.SemaphoreType.DMA((2,)),
            pltpu.SemaphoreType.DMA((n - 1, 2)),
            pltpu.SemaphoreType.DMA((n - 1,)),
        ],
        compiler_params=pltpu.CompilerParams(collective_id=0, has_side_effects=True),
    )(span_order, self_queries, self_keys, self_values, cross_queries, cross_keys, cross_values, tables)
    plain = jax.ShapeDtypeStruct((rows, width), jnp.bfloat16)
    return pl.pallas_call(
        flush,
        out_shape=(plain, plain),
        in_specs=[pl.BlockSpec(memory_space=pltpu.VMEM)] * 2,
        out_specs=(anywhere, anywhere),
        scratch_shapes=[pltpu.SemaphoreType.DMA((2,))],
    )(*[pltpu.with_memory_space_constraint(array, pltpu.VMEM) for array in held])


def fast_axis(mesh, n):
    line = mesh.devices[0, :, 0]
    coords = [getattr(device, "coords", None) for device in line]
    if any(c is None for c in coords):
        return 1
    nx = len({c[0] for c in coords})
    return nx if n % nx == 0 else 1


def solution(mesh):
    n = mesh.shape["context"]
    both = P(("groups", "context"), "tensor")
    return jax.shard_map(
        functools.partial(body, n, fast_axis(mesh, n)), mesh=mesh,
        in_specs=(both,) * 6 + (P("groups"),), out_specs=(both, both), check_vma=False)
```

```python
import functools
import math

import jax
import jax.numpy as jnp
import numpy as np
from jax import lax
from jax.experimental import pallas as pl
from jax.experimental.pallas import tpu as pltpu
from jax.sharding import PartitionSpec as P

HEAD_DIM = 128
HEADS = 16
KV_HEADS = 4
GROUP = HEADS // KV_HEADS
NEG_FILL = -1e30
SCALE = HEAD_DIM ** (-0.5) * math.log2(math.e)


def rotary_tables(spans, span_len):
    half = HEAD_DIM // 2
    frequency = 500000.0 ** (-(np.arange(half) * 2.0) / HEAD_DIM)
    frequency = np.concatenate([frequency, frequency])
    base = (np.arange(spans) * span_len)[:, None] * frequency[None, :]
    inner = np.arange(span_len)[:, None] * frequency[None, :]
    sign = np.where(np.arange(HEAD_DIM) < half, -1.0, 1.0)[None, :]
    inners = [np.cos(inner), np.sin(inner), np.cos(inner) * sign, np.sin(inner) * sign]
    return np.concatenate(inners + [np.cos(base), np.sin(base)]).astype(np.float32)


def doubling(order):
    held, steps = [0], []
    for mask in order:
        steps.append((mask, list(held)))
        held += [item ^ mask for item in held]
    return steps


def kernel(
    n, nx,
    order_hbm, q_hbm, k_hbm, v_hbm, cq_hbm, ck_hbm, cv_hbm, tables_hbm,
    out_v, cout_v,
    text, image, qs, tables, q_rot, peak, total, mixed, order,
    load_sem, send_sem, text_recv, image_recv, mate_recv, ready,
):
    me = lax.axis_index("context")
    rows = qs.shape[1]
    span_len = rows // 2
    kv_local = text.shape[3] // HEAD_DIM
    image_rows = image.shape[3]
    paired = image.shape[1] == 2
    core = lax.axis_index("tensor") if paired else 0
    z, x = me // nx, me % nx

    x_masks = [1 << b for b in reversed(range(nx.bit_length() - 1))]
    z_masks = [nx << b for b in reversed(range((n // nx).bit_length() - 1))]
    masks = z_masks + x_masks
    z_x = doubling(z_masks + x_masks)
    z_x_z = doubling(z_masks[:1] + x_masks + z_masks[1:])
    x_z = doubling(x_masks + z_masks)
    part_steps = (z_x, z_x)
    image_steps = x_z

    def flipped(index, item):
        for mask in masks:
            bit = (item // mask) % 2
            index = index + mask * bit * (1 - 2 * ((index // mask) % 2))
        return index

    partner = {mask: flipped(me, mask) for mask in (range(1, n) if paired else masks)}

    barrier = pltpu.get_barrier_semaphore()

    def hail(sem, where):
        pl.semaphore_signal(sem, inc=1, device_id=where, device_id_type=pl.DeviceIdType.MESH)

    def greet():
        if not paired:
            for mask in masks:
                hail(barrier, {"context": partner[mask]})
            return
        hail(barrier, {"tensor": 1 - core})
        hail(barrier, {"context": partner[1]})
        hail(barrier, {"context": partner[2]})

        @pl.when(z == 0)
        def _():
            hail(barrier, {"context": me + 2 * nx})

        @pl.when(z == 1)
        def _():
            hail(barrier, {"context": me + nx})
            hail(barrier, {"context": me + 2 * nx})

        @pl.when(z == 2)
        def _():
            hail(barrier, {"context": me - nx})

    def meet():
        if not paired:
            pl.semaphore_wait(barrier, len(masks))
            return
        pl.semaphore_wait(barrier, 3 + jnp.where(z == 0, 0, jnp.where(z == 2, 2, 1)))

        @pl.when(z == 1)
        def _():
            hail(ready.at[0], {"context": me - nx})

        @pl.when(z == 2)
        def _():
            hail(ready.at[0], {"context": me - nx})
            hail(ready.at[0], {"context": me + nx})

    greet()
    kv_loads = [
        pltpu.make_async_copy(k_hbm, text.at[0, 0], load_sem.at[0]),
        pltpu.make_async_copy(v_hbm, text.at[0, 1], load_sem.at[0]),
        pltpu.make_async_copy(ck_hbm, image.at[0, core, 0], load_sem.at[1]),
        pltpu.make_async_copy(cv_hbm, image.at[0, core, 1], load_sem.at[1]),
    ]
    other_loads = [
        pltpu.make_async_copy(order_hbm, order, load_sem.at[2]),
        pltpu.make_async_copy(tables_hbm, tables, load_sem.at[3]),
        pltpu.make_async_copy(q_hbm, qs.at[0], load_sem.at[4]),
        pltpu.make_async_copy(cq_hbm, qs.at[1], load_sem.at[4]),
    ]

    def landed(ref, sem):
        pltpu.make_async_copy(ref, ref, sem).wait()

    for load in kv_loads:
        load.start()
    for load in other_loads:
        load.start()
    landed(text.at[0], load_sem.at[0])
    landed(image.at[0, core], load_sem.at[1])
    meet()

    def text_copy(item, part, mask):
        return pltpu.make_async_remote_copy(
            src_ref=text.at[item, part], dst_ref=text.at[item ^ mask, part],
            send_sem=send_sem.at[0], recv_sem=text_recv.at[(item ^ mask) - 1, part],
            device_id={"context": partner[mask]}, device_id_type=pl.DeviceIdType.MESH)

    def image_copy(item, mask):
        return pltpu.make_async_remote_copy(
            src_ref=image.at[item], dst_ref=image.at[item ^ mask],
            send_sem=send_sem.at[1], recv_sem=image_recv.at[(item ^ mask) - 1],
            device_id={"context": partner[mask]}, device_id_type=pl.DeviceIdType.MESH)

    def forward_text(item, part):
        for mask, held in part_steps[part]:
            if item in held:
                text_copy(item, part, mask).start()

    def forward_image(item):
        for mask, held in image_steps:
            if item in held:
                image_copy(item, mask).start()

    def arrive_text(item, part):
        text_copy(item ^ masks[0], part, masks[0]).wait_recv()
        forward_text(item, part)

    def arrive_image(item):
        image_copy(item ^ masks[0], masks[0]).wait_recv()
        forward_image(item)

    def send(kind, item, mask, cond=None):
        copy = image_copy(item, mask) if kind == 2 else text_copy(item, kind, mask)
        if cond is None:
            copy.start()
        else:
            pl.when(cond)(copy.start)

    def pick(*values):
        result = values[-1]
        for at in range(len(values) - 2, -1, -1):
            result = jnp.where(z == at, values[at], result)
        return result

    def relayed(item, part, after):
        return pltpu.make_async_remote_copy(
            src_ref=text.at[item, part], dst_ref=text.at[item + after, part],
            send_sem=send_sem.at[0], recv_sem=text_recv.at[item + after - 1, part],
            device_id={"context": partner[1]}, device_id_type=pl.DeviceIdType.MESH)

    def relay(at):
        for part in range(2):
            relayed(places[at], part, 0).wait_recv()
            relayed(places[at], part, 1).start()
            if at < 2:
                send(part, 4, 2, z == 2 * at)

    def take(kind, item):
        if kind == 2:
            image_copy(item ^ 1, 1).wait_recv()
        else:
            relayed(item, kind, 0).wait_recv()

    def handed(item, where):
        return pltpu.make_async_remote_copy(
            src_ref=image.at[item, 0], dst_ref=image.at[item, 0],
            send_sem=send_sem.at[2], recv_sem=image_recv.at[item - 1] if item else mate_recv.at[0],
            device_id={"tensor": where}, device_id_type=pl.DeviceIdType.MESH)

    def carry(items):
        for item in items:
            take(2, item)
            handed(item, 0).start()

    def on_core(which):
        return pl.when(core == which)

    if paired:
        places = [pick(4, 2, 6, 2), pick(6, 4, 4, 4), pick(2, 6, 2, 6)]
        for part in range(2):
            send(part, 0, 1)
            send(part, 0, 2, z != 3)
            send(part, 0, 6, z == 1)
            send(part, 0, 4, z == 2)
        on_core(0)(handed(0, 1).start)

        @pl.when(z != 2)
        def _():
            pl.semaphore_wait(ready.at[0], 1)

        for mask, cond in ((6, z == 3), (2, z == 3), (4, z != 2)):
            for part in range(2):
                send(part, 0, mask, cond)

        @on_core(1)
        def _():
            handed(0, 0).wait_recv()
            send(2, 0, 1)
    else:
        forward_text(0, 0)
        forward_text(0, 1)
        forward_image(0)

    other_loads[0].wait()
    other_loads[1].wait()
    landed(qs, load_sem.at[4])

    spans = order.shape[0]

    def angles(place):
        inners = [tables[at * span_len:(at + 1) * span_len, :] for at in range(4)]
        cosines, sines, starts = [], [], []
        for part in range(2):
            span = order[2 * place + part]
            base_cos = tables[pl.ds(4 * span_len + span, 1), :]
            base_sin = tables[pl.ds(4 * span_len + spans + span, 1), :]
            cosines.append(base_cos * inners[0] - base_sin * inners[1])
            sines.append(base_sin * inners[2] + base_cos * inners[3])
            starts.append(span * span_len)
        return jnp.concatenate(cosines, 0), jnp.concatenate(sines, 0), starts

    def rotate(values, cosine, sine):
        values = values.astype(jnp.float32)
        turned = pltpu.roll(values, HEAD_DIM // 2, 1)
        return (values * cosine + turned * sine).astype(jnp.bfloat16)

    def positions(starts, shape, axis):
        index = lax.broadcasted_iota(jnp.int32, shape, axis)
        result = starts[0] + index
        for at in range(1, len(starts)):
            result = jnp.where(index < at * span_len, result, starts[at] + index - at * span_len)
        return result

    own_cos, own_sin, own_starts = angles(me)
    own_places = positions(own_starts, (rows, 1), 0)
    for head in range(kv_local * GROUP):
        q_rot[head // GROUP, pl.ds(head % GROUP * rows, rows), :] = rotate(
            qs[0, :, head * HEAD_DIM:(head + 1) * HEAD_DIM], own_cos, own_sin)

    def dot_nt(a, b):
        return lax.dot_general(a, b, (((1,), (1,)), ((), ())), preferred_element_type=jnp.float32)

    def join(pieces):
        return pieces[0] if len(pieces) == 1 else jnp.concatenate(pieces, 0)

    def block(items, first=False, last=False):
        parts = [angles(flipped(me, item)) for item in items]
        cosine, sine = join([p[0] for p in parts]), join([p[1] for p in parts])
        width = rows * len(items)
        allowed = positions(sum([p[2] for p in parts], []), (1, width), 1) <= own_places
        for head in range(kv_local):
            columns = slice(head * HEAD_DIM, (head + 1) * HEAD_DIM)
            keys = rotate(join([text[item, 0, :, columns] for item in items]), cosine, sine)
            scores = dot_nt(q_rot[head], keys) * SCALE
            scores = jnp.where(allowed[None], scores.reshape(GROUP, rows, width), NEG_FILL)
            scores = scores.reshape(GROUP * rows, width)
            top = jnp.max(scores, -1, keepdims=True)
            if not first:
                old = peak[head]
                top = jnp.maximum(top, old)
            weights = jnp.exp2(scores - top)
            summed = jnp.sum(weights, -1, keepdims=True)
            product = jnp.dot(
                weights.astype(jnp.bfloat16), join([text[item, 1, :, columns] for item in items]),
                preferred_element_type=jnp.float32)
            if not first:
                factor = jnp.exp2(old - top)
                summed = summed + total[head] * factor
                product = product + mixed[head] * factor
            if last:
                store(out_v, head, product / summed)
            else:
                peak[head] = top
                total[head] = summed
                mixed[head] = product

    def store(target, head, result):
        result = result.astype(jnp.bfloat16)
        for g in range(GROUP):
            at = head * GROUP + g
            target[:, at * HEAD_DIM:(at + 1) * HEAD_DIM] = result[g * rows:(g + 1) * rows]

    def cross():
        keys_all = image[:, core, 0].astype(jnp.float32).reshape(n * image_rows, -1).astype(jnp.bfloat16)
        values_all = image[:, core, 1].astype(jnp.float32).reshape(n * image_rows, -1).astype(jnp.bfloat16)
        for head in range(kv_local):
            columns = slice(head * HEAD_DIM, (head + 1) * HEAD_DIM)
            queries = jnp.concatenate(
                [qs[1, :, h * HEAD_DIM:(h + 1) * HEAD_DIM] for h in range(head * GROUP, (head + 1) * GROUP)], 0)
            scores = dot_nt(queries, keys_all[:, columns]) * SCALE
            weights = jnp.exp2(scores - jnp.max(scores, -1, keepdims=True))
            summed = jnp.sum(weights, -1, keepdims=True)
            product = jnp.dot(
                weights.astype(jnp.bfloat16), values_all[:, columns], preferred_element_type=jnp.float32)
            store(cout_v, head, product / summed)

    def image_start(item):
        send(2, item, 6, z == 3)
        send(2, item, 4)
        send(2, item, 2)
        send(2, item, 6, z == 1)

    block([0], first=True)
    if paired:
        for part in range(2):
            take(part, 1)
        block([1])
        relay(0)
        relay(1)

        @on_core(1)
        def _():
            image_start(0)

        relay(2)

        @on_core(1)
        def _():
            carry([1])
            image_start(1)

        block(places)

        @on_core(1)
        def _():
            for item in (4, 5):
                carry([item])
                send(2, item, 2, z % 2 == 0)

        for at in range(2):
            for part in range(2):
                take(part, places[at] + 1)
        block([places[0] + 1, places[1] + 1])

        @on_core(1)
        def _():
            carry([2, 3, 6, 7])

        for part in range(2):
            take(part, places[2] + 1)
        block([places[2] + 1], last=True)

        @on_core(0)
        def _():
            for item in range(1, n):
                handed(item, 0).wait_recv()

        cross()

        @on_core(0)
        def _():
            handed(0, 1).wait_send()

        @on_core(1)
        def _():
            landed(image.at[pl.ds(0, n - 1)], send_sem.at[1])
            landed(image.at[pl.ds(0, n - 1), 0], send_sem.at[2])
    else:
        for part in range(2):
            for mask, held in part_steps[part]:
                for item in held:
                    arrive_text(item ^ mask, part)
        for mask, held in image_steps:
            for item in held:
                arrive_image(item ^ mask)

        def step(item, unused):
            block([item])
            return 0

        lax.fori_loop(1, n, step, 0)
        for head in range(kv_local):
            store(out_v, head, mixed[head] / total[head])
        cross()
        landed(image.at[pl.ds(0, n - 1)], send_sem.at[1])
    landed(text.at[pl.ds(0, n - 1)], send_sem.at[0])


def flush(self_v, cross_v, self_hbm, cross_hbm, sems):
    copies = [
        pltpu.make_async_copy(self_v, self_hbm, sems.at[0]),
        pltpu.make_async_copy(cross_v, cross_hbm, sems.at[1]),
    ]
    for copy in copies:
        copy.start()
    for copy in copies:
        copy.wait()


def body(n, nx, cores, self_queries, self_keys, self_values, cross_queries, cross_keys, cross_values, span_order):
    rows, width = self_queries.shape
    kv_width = self_keys.shape[1]
    kv_local = kv_width // HEAD_DIM
    image_rows = cross_keys.shape[0]
    tables = rotary_tables(span_order.shape[0], rows // 2)
    anywhere = pl.BlockSpec(memory_space=pl.ANY)
    result = pltpu.VMEM((rows, width), jnp.bfloat16)
    held = pl.pallas_call(
        functools.partial(kernel, n, nx),
        out_shape=(result, result),
        in_specs=[anywhere] * 8,
        out_specs=(pl.BlockSpec(memory_space=pltpu.VMEM),) * 2,
        scratch_shapes=[
            pltpu.VMEM((n, 2, rows, kv_width), jnp.bfloat16),
            pltpu.VMEM((n, cores, 2, image_rows, kv_width), jnp.bfloat16),
            pltpu.VMEM((2, rows, width), jnp.bfloat16),
            pltpu.VMEM(tables.shape, jnp.float32),
            pltpu.VMEM((kv_local, GROUP * rows, HEAD_DIM), jnp.bfloat16),
            pltpu.VMEM((kv_local, GROUP * rows, 1), jnp.float32),
            pltpu.VMEM((kv_local, GROUP * rows, 1), jnp.float32),
            pltpu.VMEM((kv_local, GROUP * rows, HEAD_DIM), jnp.float32),
            pltpu.SMEM(span_order.shape, jnp.int32),
            pltpu.SemaphoreType.DMA((5,)),
            pltpu.SemaphoreType.DMA((3,)),
            pltpu.SemaphoreType.DMA((n - 1, 2)),
            pltpu.SemaphoreType.DMA((n - 1,)),
            pltpu.SemaphoreType.DMA((1,)),
            pltpu.SemaphoreType.REGULAR((1,)),
        ],
        compiler_params=pltpu.CompilerParams(collective_id=0, has_side_effects=True),
    )(span_order, self_queries, self_keys, self_values, cross_queries, cross_keys, cross_values, tables)
    plain = jax.ShapeDtypeStruct((rows, width), jnp.bfloat16)
    return pl.pallas_call(
        flush,
        out_shape=(plain, plain),
        in_specs=[pl.BlockSpec(memory_space=pltpu.VMEM)] * 2,
        out_specs=(anywhere, anywhere),
        scratch_shapes=[pltpu.SemaphoreType.DMA((2,))],
    )(*[pltpu.with_memory_space_constraint(array, pltpu.VMEM) for array in held])


def fast_axis(mesh, n):
    line = mesh.devices[0, :, 0]
    coords = [getattr(device, "coords", None) for device in line]
    if any(c is None for c in coords):
        return 1
    nx = len({c[0] for c in coords})
    return nx if n % nx == 0 else 1


def solution(mesh):
    n = mesh.shape["context"]
    nx = fast_axis(mesh, n)
    cores = 2 if (n, nx, mesh.shape["tensor"]) == (8, 2, 2) else 1
    both = P(("groups", "context"), "tensor")
    return jax.shard_map(
        functools.partial(body, n, nx, cores), mesh=mesh,
        in_specs=(both,) * 6 + (P("groups"),), out_specs=(both, both), check_vma=False)
```

```python
import functools
import math

import jax
import jax.numpy as jnp
import numpy as np
from jax import lax
from jax.experimental import pallas as pl
from jax.experimental.pallas import tpu as pltpu
from jax.sharding import PartitionSpec as P

HEAD_DIM = 128
HEADS = 16
KV_HEADS = 4
GROUP = HEADS // KV_HEADS
NEG_FILL = -1e30
DIRECT = (2, 3, 6, 7)
SCALE = HEAD_DIM ** (-0.5) * math.log2(math.e)


def rotary_tables(spans, span_len):
    half = HEAD_DIM // 2
    frequency = 500000.0 ** (-(np.arange(half) * 2.0) / HEAD_DIM)
    frequency = np.concatenate([frequency, frequency])
    base = (np.arange(spans) * span_len)[:, None] * frequency[None, :]
    inner = np.arange(span_len)[:, None] * frequency[None, :]
    sign = np.where(np.arange(HEAD_DIM) < half, -1.0, 1.0)[None, :]
    inners = [np.cos(inner), np.sin(inner), np.cos(inner) * sign, np.sin(inner) * sign]
    return np.concatenate(inners + [np.cos(base), np.sin(base)]).astype(np.float32)


def doubling(order):
    held, steps = [0], []
    for mask in order:
        steps.append((mask, list(held)))
        held += [item ^ mask for item in held]
    return steps


def kernel(
    n, nx,
    order_hbm, q_hbm, k_hbm, v_hbm, cq_hbm, ck_hbm, cv_hbm, tables_hbm,
    out_v, cout_v,
    text, image, qs, tables, q_rot, gap, peak, total, mixed, order,
    load_sem, send_sem, text_recv, image_recv, mate_recv, ready,
):
    me = lax.axis_index("context")
    rows = qs.shape[1]
    span_len = rows // 2
    kv_local = text.shape[3] // HEAD_DIM
    image_rows = image.shape[3]
    paired = image.shape[1] == 2
    core = lax.axis_index("tensor") if paired else 0
    z, x = me // nx, me % nx

    x_masks = [1 << b for b in reversed(range(nx.bit_length() - 1))]
    z_masks = [nx << b for b in reversed(range((n // nx).bit_length() - 1))]
    masks = z_masks + x_masks
    z_x = doubling(z_masks + x_masks)
    z_x_z = doubling(z_masks[:1] + x_masks + z_masks[1:])
    x_z = doubling(x_masks + z_masks)
    part_steps = (z_x, z_x)
    image_steps = x_z

    def flipped(index, item):
        for mask in masks:
            bit = (item // mask) % 2
            index = index + mask * bit * (1 - 2 * ((index // mask) % 2))
        return index

    partner = {mask: flipped(me, mask) for mask in (range(1, n) if paired else masks)}

    barrier = pltpu.get_barrier_semaphore()

    def hail(sem, where):
        pl.semaphore_signal(sem, inc=1, device_id=where, device_id_type=pl.DeviceIdType.MESH)

    def greet():
        if not paired:
            for mask in masks:
                hail(barrier, {"context": partner[mask]})
            return
        hail(barrier, {"tensor": 1 - core})
        hail(barrier, {"context": partner[1]})
        hail(barrier, {"context": partner[2]})

        @pl.when(z == 0)
        def _():
            hail(barrier, {"context": me + 2 * nx})

        @pl.when(z == 1)
        def _():
            hail(barrier, {"context": me + nx})
            hail(barrier, {"context": me + 2 * nx})

        @pl.when(z == 2)
        def _():
            hail(barrier, {"context": me - nx})

    def meet():
        if not paired:
            pl.semaphore_wait(barrier, len(masks))
            return
        pl.semaphore_wait(barrier, 3 + jnp.where(z == 0, 0, jnp.where(z == 2, 2, 1)))

        @pl.when(z == 1)
        def _():
            hail(ready.at[0], {"context": me - nx})

        @pl.when(z == 2)
        def _():
            hail(ready.at[0], {"context": me - nx})
            hail(ready.at[0], {"context": me + nx})

        @pl.when(jnp.logical_and(z == 2, core == 0))
        def _():
            hail(ready.at[1], {"tensor": 1})

    greet()
    kv_loads = [
        pltpu.make_async_copy(k_hbm, text.at[0, 0], load_sem.at[0]),
        pltpu.make_async_copy(v_hbm, text.at[0, 1], load_sem.at[0]),
        pltpu.make_async_copy(ck_hbm, image.at[0, core, 0], load_sem.at[1]),
        pltpu.make_async_copy(cv_hbm, image.at[0, core, 1], load_sem.at[1]),
    ]
    other_loads = [
        pltpu.make_async_copy(order_hbm, order, load_sem.at[2]),
        pltpu.make_async_copy(tables_hbm, tables, load_sem.at[3]),
        pltpu.make_async_copy(q_hbm, qs.at[0], load_sem.at[4]),
        pltpu.make_async_copy(cq_hbm, qs.at[1], load_sem.at[4]),
    ]

    def landed(ref, sem):
        pltpu.make_async_copy(ref, ref, sem).wait()

    for load in kv_loads:
        load.start()
    for load in other_loads:
        load.start()
    landed(text.at[0], load_sem.at[0])
    landed(image.at[0, core], load_sem.at[1])
    meet()

    def text_copy(item, part, mask):
        return pltpu.make_async_remote_copy(
            src_ref=text.at[item, part], dst_ref=text.at[item ^ mask, part],
            send_sem=send_sem.at[0], recv_sem=text_recv.at[(item ^ mask) - 1, part],
            device_id={"context": partner[mask]}, device_id_type=pl.DeviceIdType.MESH)

    def image_copy(item, mask):
        return pltpu.make_async_remote_copy(
            src_ref=image.at[item], dst_ref=image.at[item ^ mask],
            send_sem=send_sem.at[1], recv_sem=image_recv.at[(item ^ mask) - 1],
            device_id={"context": partner[mask]}, device_id_type=pl.DeviceIdType.MESH)

    def forward_text(item, part):
        for mask, held in part_steps[part]:
            if item in held:
                text_copy(item, part, mask).start()

    def forward_image(item):
        for mask, held in image_steps:
            if item in held:
                image_copy(item, mask).start()

    def arrive_text(item, part):
        text_copy(item ^ masks[0], part, masks[0]).wait_recv()
        forward_text(item, part)

    def arrive_image(item):
        image_copy(item ^ masks[0], masks[0]).wait_recv()
        forward_image(item)

    def send(kind, item, mask, cond=None):
        if kind == 2 and (item ^ mask) in DIRECT:
            copies = [straight(item, item ^ mask, half, partner[mask]) for half in range(2)]
        else:
            copies = [image_copy(item, mask) if kind == 2 else text_copy(item, kind, mask)]
        for copy in copies:
            if cond is None:
                copy.start()
            else:
                pl.when(cond)(copy.start)

    def straight(item, to, half, where):
        return pltpu.make_async_remote_copy(
            src_ref=image.at[item, half], dst_ref=image.at[to, half],
            send_sem=send_sem.at[1], recv_sem=image_recv.at[to - 1],
            device_id={"context": where, "tensor": half}, device_id_type=pl.DeviceIdType.MESH)

    def pick(*values):
        result = values[-1]
        for at in range(len(values) - 2, -1, -1):
            result = jnp.where(z == at, values[at], result)
        return result

    def relayed(item, part, after):
        return pltpu.make_async_remote_copy(
            src_ref=text.at[item, part], dst_ref=text.at[item + after, part],
            send_sem=send_sem.at[0], recv_sem=text_recv.at[item + after - 1, part],
            device_id={"context": partner[1]}, device_id_type=pl.DeviceIdType.MESH)

    def relay(at):
        for part in range(2):
            relayed(places[at], part, 0).wait_recv()
            relayed(places[at], part, 1).start()
            if at < 2:
                send(part, 4, 2, z == 2 * at)

    def take(kind, item):
        if kind == 2 and item in DIRECT:
            straight(item, item, 1, partner[1]).wait_recv()
        elif kind == 2:
            image_copy(item ^ 1, 1).wait_recv()
        else:
            relayed(item, kind, 0).wait_recv()

    def handed(item, where):
        return pltpu.make_async_remote_copy(
            src_ref=image.at[item, 0], dst_ref=image.at[item, 0],
            send_sem=send_sem.at[2], recv_sem=image_recv.at[item - 1] if item else mate_recv.at[0],
            device_id={"tensor": where}, device_id_type=pl.DeviceIdType.MESH)

    def carry(items):
        for item in items:
            take(2, item)
            if item not in DIRECT:
                handed(item, 0).start()

    def on_core(which):
        return pl.when(core == which)

    if paired:
        places = [pick(4, 2, 6, 2), pick(6, 4, 4, 4), pick(2, 6, 2, 6)]
        for part in range(2):
            send(part, 0, 1)
            send(part, 0, 2, z != 3)
            send(part, 0, 6, z == 1)
            send(part, 0, 4, z == 2)
        on_core(0)(handed(0, 1).start)

        @pl.when(z != 2)
        def _():
            pl.semaphore_wait(ready.at[0], 1)

        for mask, cond in ((6, z == 3), (2, z == 3), (4, z != 2)):
            for part in range(2):
                send(part, 0, mask, cond)

        @on_core(1)
        def _():
            handed(0, 0).wait_recv()
            send(2, 0, 1)

            @pl.when(z == 2)
            def _():
                pl.semaphore_wait(ready.at[1], 1)
                hail(ready.at[1], {"context": me + nx})
    else:
        forward_text(0, 0)
        forward_text(0, 1)
        forward_image(0)

    other_loads[0].wait()
    other_loads[1].wait()
    landed(qs, load_sem.at[4])

    spans = order.shape[0]

    def angles(place):
        inners = [tables[at * span_len:(at + 1) * span_len, :] for at in range(4)]
        cosines, sines, starts = [], [], []
        for part in range(2):
            span = order[2 * place + part]
            base_cos = tables[pl.ds(4 * span_len + span, 1), :]
            base_sin = tables[pl.ds(4 * span_len + spans + span, 1), :]
            cosines.append(base_cos * inners[0] - base_sin * inners[1])
            sines.append(base_sin * inners[2] + base_cos * inners[3])
            starts.append(span * span_len)
        return jnp.concatenate(cosines, 0), jnp.concatenate(sines, 0), starts

    def rotate(values, cosine, sine):
        values = values.astype(jnp.float32)
        turned = pltpu.roll(values, HEAD_DIM // 2, 1)
        return (values * cosine + turned * sine).astype(jnp.bfloat16)

    own_cos, own_sin, own_starts = angles(me)
    lane = lax.broadcasted_iota(jnp.int32, gap.shape, 1)
    for g in range(1, GROUP):
        lane = jnp.where(lane >= rows, lane - rows, lane)
    own_places = jnp.where(lane < span_len, own_starts[0] + lane, own_starts[1] + lane - span_len)
    gap[...] = own_places - lax.broadcasted_iota(jnp.int32, gap.shape, 0)
    for head in range(kv_local * GROUP):
        q_rot[head // GROUP, pl.ds(head % GROUP * rows, rows), :] = rotate(
            qs[0, :, head * HEAD_DIM:(head + 1) * HEAD_DIM], own_cos, own_sin)

    def dot_nt(a, b):
        return lax.dot_general(a, b, (((1,), (1,)), ((), ())), preferred_element_type=jnp.float32)

    def join(pieces):
        return pieces[0] if len(pieces) == 1 else jnp.concatenate(pieces, 0)

    def mix(values, weights):
        return lax.dot_general(
            values, weights.astype(jnp.bfloat16), (((0,), (0,)), ((), ())), preferred_element_type=jnp.float32)

    def folded(weights):
        return jnp.sum(weights.reshape(-1, 8, weights.shape[1]), 0)

    heads = range(kv_local)
    head_columns = [slice(head * HEAD_DIM, (head + 1) * HEAD_DIM) for head in heads]

    def block(items, first=False, last=False):
        parts = [angles(flipped(me, item)) for item in items]
        cosine, sine = join([p[0] for p in parts]), join([p[1] for p in parts])
        starts = sum([p[2] for p in parts], [])
        keys = [rotate(join([text[item, 0, :, at] for item in items]), cosine, sine) for at in head_columns]
        scores = [dot_nt(keys[head], q_rot[head]) for head in heads]
        scores = [join([
            jnp.where(gap[...] >= starts[at], block_scores[at * span_len:(at + 1) * span_len], NEG_FILL)
            for at in range(len(starts))]) for block_scores in scores]
        top = [jnp.max(block_scores, 0, keepdims=True) for block_scores in scores]
        if not first:
            old = [peak[head] for head in heads]
            top = [jnp.maximum(top[head], old[head]) for head in heads]
        weights = [jnp.exp2((scores[head] - top[head]) * SCALE) for head in heads]
        values = [join([text[item, 1, :, at] for item in items]) for at in head_columns]
        product = [mix(values[head], weights[head]) for head in heads]
        summed = [folded(weights[head]) for head in heads]
        if not first:
            factor = [jnp.exp2((old[head] - top[head]) * SCALE) for head in heads]
            summed = [summed[head] + total[head] * factor[head] for head in heads]
            product = [product[head] + mixed[head] * factor[head] for head in heads]
        if last:
            store(out_v, product, summed)
            return
        for head in heads:
            peak[head] = top[head]
            total[head] = summed[head]
            mixed[head] = product[head]

    def store(target, product, summed):
        result = [
            (product[head] * (1.0 / jnp.sum(summed[head], 0, keepdims=True))).T.astype(jnp.bfloat16) for head in heads]
        for head in heads:
            for g in range(GROUP):
                at = head * GROUP + g
                target[:, at * HEAD_DIM:(at + 1) * HEAD_DIM] = result[head][g * rows:(g + 1) * rows]

    def cross():
        keys_all = image[:, core, 0].astype(jnp.float32).reshape(n * image_rows, -1).astype(jnp.bfloat16)
        values_all = image[:, core, 1].astype(jnp.float32).reshape(n * image_rows, -1).astype(jnp.bfloat16)
        queries = [
            jnp.concatenate(
                [qs[1, :, h * HEAD_DIM:(h + 1) * HEAD_DIM] for h in range(head * GROUP, (head + 1) * GROUP)], 0)
            for head in heads]
        scores = [dot_nt(keys_all[:, head_columns[head]], queries[head]) for head in heads]
        top = [jnp.max(scores[head], 0, keepdims=True) for head in heads]
        weights = [jnp.exp2((scores[head] - top[head]) * SCALE) for head in heads]
        product = [mix(values_all[:, head_columns[head]], weights[head]) for head in heads]
        store(cout_v, product, [folded(weights[head]) for head in heads])

    def image_start(item):
        send(2, item, 6, z == 3)
        send(2, item, 4, z != 1)
        send(2, item, 2)
        send(2, item, 6, z == 1)

    block([0], first=True)
    if paired:
        for part in range(2):
            take(part, 1)
        block([1])
        relay(0)
        relay(1)

        @on_core(1)
        def _():
            @pl.when(z == 3)
            def _():
                pl.semaphore_wait(ready.at[1], 1)

            image_start(0)

        relay(2)

        @on_core(1)
        def _():
            carry([1])
            image_start(1)

        block(places)

        @on_core(1)
        def _():
            for item in range(2):
                send(2, item, 4, z == 1)

        @on_core(1)
        def _():
            for item in (4, 5):
                carry([item])
                send(2, item, 2, z % 2 == 0)

        for at in range(2):
            for part in range(2):
                take(part, places[at] + 1)
        block([places[0] + 1, places[1] + 1])

        def finish():
            @on_core(0)
            def _():
                for item in range(1, n):
                    handed(item, 0).wait_recv()

            @on_core(1)
            def _():
                carry([2, 3, 6, 7])

            cross()

        soon = jnp.logical_and(core == 0, z > 0)
        pl.when(soon)(finish)
        for part in range(2):
            take(part, places[2] + 1)
        block([places[2] + 1], last=True)
        pl.when(jnp.logical_not(soon))(finish)

        @on_core(0)
        def _():
            handed(0, 1).wait_send()

        @on_core(1)
        def _():
            landed(image.at[pl.ds(0, n - 1)], send_sem.at[1])
            landed(image.at[pl.ds(0, n - 1 - len(DIRECT)), 0], send_sem.at[2])
    else:
        for part in range(2):
            for mask, held in part_steps[part]:
                for item in held:
                    arrive_text(item ^ mask, part)
        for mask, held in image_steps:
            for item in held:
                arrive_image(item ^ mask)

        def step(item, unused):
            block([item])
            return 0

        lax.fori_loop(1, n, step, 0)
        store(out_v, [mixed[head] for head in heads], [total[head] for head in heads])
        cross()
        landed(image.at[pl.ds(0, n - 1)], send_sem.at[1])
    landed(text.at[pl.ds(0, n - 1)], send_sem.at[0])


def flush(self_v, cross_v, self_hbm, cross_hbm, sems):
    copies = [
        pltpu.make_async_copy(self_v, self_hbm, sems.at[0]),
        pltpu.make_async_copy(cross_v, cross_hbm, sems.at[1]),
    ]
    for copy in copies:
        copy.start()
    for copy in copies:
        copy.wait()


def body(n, nx, cores, self_queries, self_keys, self_values, cross_queries, cross_keys, cross_values, span_order):
    rows, width = self_queries.shape
    kv_width = self_keys.shape[1]
    kv_local = kv_width // HEAD_DIM
    image_rows = cross_keys.shape[0]
    tables = rotary_tables(span_order.shape[0], rows // 2)
    anywhere = pl.BlockSpec(memory_space=pl.ANY)
    result = pltpu.VMEM((rows, width), jnp.bfloat16)
    held = pl.pallas_call(
        functools.partial(kernel, n, nx),
        out_shape=(result, result),
        in_specs=[anywhere] * 8,
        out_specs=(pl.BlockSpec(memory_space=pltpu.VMEM),) * 2,
        scratch_shapes=[
            pltpu.VMEM((n, 2, rows, kv_width), jnp.bfloat16),
            pltpu.VMEM((n, cores, 2, image_rows, kv_width), jnp.bfloat16),
            pltpu.VMEM((2, rows, width), jnp.bfloat16),
            pltpu.VMEM(tables.shape, jnp.float32),
            pltpu.VMEM((kv_local, GROUP * rows, HEAD_DIM), jnp.bfloat16),
            pltpu.VMEM((rows // 2, GROUP * rows), jnp.int32),
            pltpu.VMEM((kv_local, 1, GROUP * rows), jnp.float32),
            pltpu.VMEM((kv_local, 8, GROUP * rows), jnp.float32),
            pltpu.VMEM((kv_local, HEAD_DIM, GROUP * rows), jnp.float32),
            pltpu.SMEM(span_order.shape, jnp.int32),
            pltpu.SemaphoreType.DMA((5,)),
            pltpu.SemaphoreType.DMA((3,)),
            pltpu.SemaphoreType.DMA((n - 1, 2)),
            pltpu.SemaphoreType.DMA((n - 1,)),
            pltpu.SemaphoreType.DMA((1,)),
            pltpu.SemaphoreType.REGULAR((2,)),
        ],
        compiler_params=pltpu.CompilerParams(collective_id=0, has_side_effects=True),
    )(span_order, self_queries, self_keys, self_values, cross_queries, cross_keys, cross_values, tables)
    plain = jax.ShapeDtypeStruct((rows, width), jnp.bfloat16)
    return pl.pallas_call(
        flush,
        out_shape=(plain, plain),
        in_specs=[pl.BlockSpec(memory_space=pltpu.VMEM)] * 2,
        out_specs=(anywhere, anywhere),
        scratch_shapes=[pltpu.SemaphoreType.DMA((2,))],
    )(*[pltpu.with_memory_space_constraint(array, pltpu.VMEM) for array in held])


def fast_axis(mesh, n):
    line = mesh.devices[0, :, 0]
    coords = [getattr(device, "coords", None) for device in line]
    if any(c is None for c in coords):
        return 1
    nx = len({c[0] for c in coords})
    return nx if n % nx == 0 else 1


def solution(mesh):
    n = mesh.shape["context"]
    nx = fast_axis(mesh, n)
    cores = 2 if (n, nx, mesh.shape["tensor"]) == (8, 2, 2) else 1
    both = P(("groups", "context"), "tensor")
    return jax.shard_map(
        functools.partial(body, n, nx, cores), mesh=mesh,
        in_specs=(both,) * 6 + (P("groups"),), out_specs=(both, both), check_vma=False)
```

```python
import functools
import math

import jax
import jax.numpy as jnp
import numpy as np
from jax import lax
from jax.experimental import pallas as pl
from jax.experimental.pallas import tpu as pltpu
from jax.sharding import PartitionSpec as P

HEAD_DIM = 128
HEADS = 16
KV_HEADS = 4
GROUP = HEADS // KV_HEADS
NEG_FILL = -1e30
DIRECT = (2, 3, 6, 7)
SCALE = HEAD_DIM ** (-0.5) * math.log2(math.e)


def rotary_tables(spans, span_len):
    half = HEAD_DIM // 2
    frequency = 500000.0 ** (-(np.arange(half) * 2.0) / HEAD_DIM)
    frequency = np.concatenate([frequency, frequency])
    base = (np.arange(spans) * span_len)[:, None] * frequency[None, :]
    inner = np.arange(span_len)[:, None] * frequency[None, :]
    sign = np.where(np.arange(HEAD_DIM) < half, -1.0, 1.0)[None, :]
    inners = [np.cos(inner), np.sin(inner), np.cos(inner) * sign, np.sin(inner) * sign]
    return np.concatenate(inners + [np.cos(base), np.sin(base)]).astype(np.float32)


def doubling(order):
    held, steps = [0], []
    for mask in order:
        steps.append((mask, list(held)))
        held += [item ^ mask for item in held]
    return steps


def kernel(
    n, nx,
    order_hbm, q_hbm, k_hbm, v_hbm, cq_hbm, ck_hbm, cv_hbm, tables_hbm,
    out_v, cout_v,
    text, image, qs, tables, q_rot, gap, peak, total, mixed, order,
    load_sem, send_sem, text_recv, image_recv, mate_recv, ready,
):
    me = lax.axis_index("context")
    rows = qs.shape[1]
    span_len = rows // 2
    kv_local = text.shape[3] // HEAD_DIM
    image_rows = image.shape[3]
    paired = image.shape[1] == 2
    core = lax.axis_index("tensor") if paired else 0
    z, x = me // nx, me % nx

    x_masks = [1 << b for b in reversed(range(nx.bit_length() - 1))]
    z_masks = [nx << b for b in reversed(range((n // nx).bit_length() - 1))]
    masks = z_masks + x_masks
    z_x = doubling(z_masks + x_masks)
    z_x_z = doubling(z_masks[:1] + x_masks + z_masks[1:])
    x_z = doubling(x_masks + z_masks)
    part_steps = (z_x, z_x)
    image_steps = x_z

    def flipped(index, item):
        for mask in masks:
            bit = (item // mask) % 2
            index = index + mask * bit * (1 - 2 * ((index // mask) % 2))
        return index

    partner = {mask: flipped(me, mask) for mask in (range(1, n) if paired else masks)}

    barrier = pltpu.get_barrier_semaphore()

    def hail(sem, where):
        pl.semaphore_signal(sem, inc=1, device_id=where, device_id_type=pl.DeviceIdType.MESH)

    def greet():
        if not paired:
            for mask in masks:
                hail(barrier, {"context": partner[mask]})
            return
        hail(barrier, {"tensor": 1 - core})
        hail(barrier, {"context": partner[1]})
        hail(barrier, {"context": partner[2]})

        @pl.when(z == 0)
        def _():
            hail(barrier, {"context": me + 2 * nx})

        @pl.when(z == 1)
        def _():
            hail(barrier, {"context": me + nx})
            hail(barrier, {"context": me + 2 * nx})

        @pl.when(z == 2)
        def _():
            hail(barrier, {"context": me - nx})

    def meet():
        if not paired:
            pl.semaphore_wait(barrier, len(masks))
            return
        pl.semaphore_wait(barrier, 3 + jnp.where(z == 0, 0, jnp.where(z == 2, 2, 1)))

        @pl.when(z == 1)
        def _():
            hail(ready.at[0], {"context": me - nx})

        @pl.when(z == 2)
        def _():
            hail(ready.at[0], {"context": me - nx})
            hail(ready.at[0], {"context": me + nx})

        @pl.when(jnp.logical_and(z == 2, core == 0))
        def _():
            hail(ready.at[1], {"tensor": 1})

    greet()
    kv_loads = [
        pltpu.make_async_copy(k_hbm, text.at[0, 0], load_sem.at[0]),
        pltpu.make_async_copy(v_hbm, text.at[0, 1], load_sem.at[0]),
        pltpu.make_async_copy(ck_hbm, image.at[0, core, 0], load_sem.at[1]),
        pltpu.make_async_copy(cv_hbm, image.at[0, core, 1], load_sem.at[1]),
    ]
    other_loads = [
        pltpu.make_async_copy(order_hbm, order, load_sem.at[2]),
        pltpu.make_async_copy(tables_hbm, tables, load_sem.at[3]),
        pltpu.make_async_copy(q_hbm, qs.at[0], load_sem.at[4]),
        pltpu.make_async_copy(cq_hbm, qs.at[1], load_sem.at[4]),
    ]

    def landed(ref, sem):
        pltpu.make_async_copy(ref, ref, sem).wait()

    for load in kv_loads:
        load.start()
    for load in other_loads:
        load.start()
    landed(text.at[0], load_sem.at[0])
    landed(image.at[0, core], load_sem.at[1])
    meet()

    def text_copy(item, part, mask):
        return pltpu.make_async_remote_copy(
            src_ref=text.at[item, part], dst_ref=text.at[item ^ mask, part],
            send_sem=send_sem.at[0], recv_sem=text_recv.at[(item ^ mask) - 1, part],
            device_id={"context": partner[mask]}, device_id_type=pl.DeviceIdType.MESH)

    def image_copy(item, mask):
        return pltpu.make_async_remote_copy(
            src_ref=image.at[item], dst_ref=image.at[item ^ mask],
            send_sem=send_sem.at[1], recv_sem=image_recv.at[(item ^ mask) - 1],
            device_id={"context": partner[mask]}, device_id_type=pl.DeviceIdType.MESH)

    def forward_text(item, part):
        for mask, held in part_steps[part]:
            if item in held:
                text_copy(item, part, mask).start()

    def forward_image(item):
        for mask, held in image_steps:
            if item in held:
                image_copy(item, mask).start()

    def arrive_text(item, part):
        text_copy(item ^ masks[0], part, masks[0]).wait_recv()
        forward_text(item, part)

    def arrive_image(item):
        image_copy(item ^ masks[0], masks[0]).wait_recv()
        forward_image(item)

    def send(kind, item, mask, cond=None):
        if kind == 2 and (item ^ mask) in DIRECT:
            copies = [straight(item, item ^ mask, half, partner[mask]) for half in range(2)]
        else:
            copies = [image_copy(item, mask) if kind == 2 else text_copy(item, kind, mask)]
        for copy in copies:
            if cond is None:
                copy.start()
            else:
                pl.when(cond)(copy.start)

    def straight(item, to, half, where):
        return pltpu.make_async_remote_copy(
            src_ref=image.at[item, half], dst_ref=image.at[to, half],
            send_sem=send_sem.at[1], recv_sem=image_recv.at[to - 1],
            device_id={"context": where, "tensor": half}, device_id_type=pl.DeviceIdType.MESH)

    def pick(*values):
        result = values[-1]
        for at in range(len(values) - 2, -1, -1):
            result = jnp.where(z == at, values[at], result)
        return result

    def relayed(item, part, after):
        return pltpu.make_async_remote_copy(
            src_ref=text.at[item, part], dst_ref=text.at[item + after, part],
            send_sem=send_sem.at[0], recv_sem=text_recv.at[item + after - 1, part],
            device_id={"context": partner[1]}, device_id_type=pl.DeviceIdType.MESH)

    def relay(at):
        for part in range(2):
            relayed(places[at], part, 0).wait_recv()
            relayed(places[at], part, 1).start()
            if at < 2:
                send(part, 4, 2, z == 2 * at)

    def take(kind, item):
        if kind == 2 and item in DIRECT:
            straight(item, item, 1, partner[1]).wait_recv()
        elif kind == 2:
            image_copy(item ^ 1, 1).wait_recv()
        else:
            relayed(item, kind, 0).wait_recv()

    def handed(item, where):
        return pltpu.make_async_remote_copy(
            src_ref=image.at[item, 0], dst_ref=image.at[item, 0],
            send_sem=send_sem.at[2], recv_sem=image_recv.at[item - 1] if item else mate_recv.at[0],
            device_id={"tensor": where}, device_id_type=pl.DeviceIdType.MESH)

    def carry(items):
        for item in items:
            take(2, item)
            if item not in DIRECT:
                handed(item, 0).start()

    def on_core(which):
        return pl.when(core == which)

    if paired:
        places = [pick(4, 2, 6, 2), pick(6, 4, 4, 4), pick(2, 6, 2, 6)]
        for part in range(2):
            send(part, 0, 1)
            send(part, 0, 2, z != 3)
            send(part, 0, 6, z == 1)
            send(part, 0, 4, z == 2)
        on_core(0)(handed(0, 1).start)

        @pl.when(z != 2)
        def _():
            pl.semaphore_wait(ready.at[0], 1)

        for mask, cond in ((6, z == 3), (2, z == 3), (4, z != 2)):
            for part in range(2):
                send(part, 0, mask, cond)

        @on_core(1)
        def _():
            handed(0, 0).wait_recv()
            send(2, 0, 1)

            @pl.when(z == 2)
            def _():
                pl.semaphore_wait(ready.at[1], 1)
                hail(ready.at[1], {"context": me + nx})
    else:
        forward_text(0, 0)
        forward_text(0, 1)
        forward_image(0)

    other_loads[0].wait()
    other_loads[1].wait()
    landed(qs, load_sem.at[4])

    spans = order.shape[0]

    def angles(place):
        inners = [tables[at * span_len:(at + 1) * span_len, :] for at in range(4)]
        cosines, sines, starts = [], [], []
        for part in range(2):
            span = order[2 * place + part]
            base_cos = tables[pl.ds(4 * span_len + span, 1), :]
            base_sin = tables[pl.ds(4 * span_len + spans + span, 1), :]
            cosines.append(base_cos * inners[0] - base_sin * inners[1])
            sines.append(base_sin * inners[2] + base_cos * inners[3])
            starts.append(span * span_len)
        return jnp.concatenate(cosines, 0), jnp.concatenate(sines, 0), starts

    def rotate(values, cosine, sine):
        values = values.astype(jnp.float32)
        turned = pltpu.roll(values, HEAD_DIM // 2, 1)
        return (values * cosine + turned * sine).astype(jnp.bfloat16)

    own_cos, own_sin, own_starts = angles(me)
    lane = lax.broadcasted_iota(jnp.int32, gap.shape, 1)
    for g in range(1, GROUP):
        lane = jnp.where(lane >= rows, lane - rows, lane)
    own_places = jnp.where(lane < span_len, own_starts[0] + lane, own_starts[1] + lane - span_len)
    gap[...] = own_places - lax.broadcasted_iota(jnp.int32, gap.shape, 0)
    for head in range(kv_local * GROUP):
        q_rot[head // GROUP, pl.ds(head % GROUP * rows, rows), :] = rotate(
            qs[0, :, head * HEAD_DIM:(head + 1) * HEAD_DIM], own_cos, own_sin)

    def dot_nt(a, b):
        return lax.dot_general(a, b, (((1,), (1,)), ((), ())), preferred_element_type=jnp.float32)

    def join(pieces):
        return pieces[0] if len(pieces) == 1 else jnp.concatenate(pieces, 0)

    def mix(values, weights):
        return lax.dot_general(
            values, weights.astype(jnp.bfloat16), (((0,), (0,)), ((), ())), preferred_element_type=jnp.float32)

    def folded(weights):
        return jnp.sum(weights.reshape(-1, 8, weights.shape[1]), 0)

    heads = range(kv_local)
    head_columns = [slice(head * HEAD_DIM, (head + 1) * HEAD_DIM) for head in heads]

    def weigh(items, first=False):
        parts = [angles(flipped(me, item)) for item in items]
        cosine, sine = join([p[0] for p in parts]), join([p[1] for p in parts])
        starts = sum([p[2] for p in parts], [])
        keys = [rotate(join([text[item, 0, :, at] for item in items]), cosine, sine) for at in head_columns]
        scores = [dot_nt(keys[head], q_rot[head]) for head in heads]
        scores = [join([
            jnp.where(gap[...] >= starts[at], block_scores[at * span_len:(at + 1) * span_len], NEG_FILL)
            for at in range(len(starts))]) for block_scores in scores]
        top = [jnp.max(block_scores, 0, keepdims=True) for block_scores in scores]
        if not first:
            old = [peak[head] for head in heads]
            top = [jnp.maximum(top[head], old[head]) for head in heads]
        weights = [jnp.exp2((scores[head] - top[head]) * SCALE) for head in heads]
        summed = [folded(weights[head]) for head in heads]
        if first:
            return top, weights, summed, None
        factor = [jnp.exp2((old[head] - top[head]) * SCALE) for head in heads]
        return top, weights, [summed[head] + total[head] * factor[head] for head in heads], factor

    def add(items, weighed, last=False):
        top, weights, summed, factor = weighed
        values = [join([text[item, 1, :, at] for item in items]) for at in head_columns]
        product = [mix(values[head], weights[head]) for head in heads]
        if factor is not None:
            product = [product[head] + mixed[head] * factor[head] for head in heads]
        if last:
            store(out_v, product, summed)
            return
        for head in heads:
            peak[head] = top[head]
            total[head] = summed[head]
            mixed[head] = product[head]

    def block(items, first=False):
        add(items, weigh(items, first))

    def store(target, product, summed):
        result = [
            (product[head] * (1.0 / jnp.sum(summed[head], 0, keepdims=True))).T.astype(jnp.bfloat16) for head in heads]
        for head in heads:
            for g in range(GROUP):
                at = head * GROUP + g
                target[:, at * HEAD_DIM:(at + 1) * HEAD_DIM] = result[head][g * rows:(g + 1) * rows]

    def cross_weigh():
        keys_all = image[:, core, 0].astype(jnp.float32).reshape(n * image_rows, -1).astype(jnp.bfloat16)
        values_all = image[:, core, 1].astype(jnp.float32).reshape(n * image_rows, -1).astype(jnp.bfloat16)
        queries = [
            jnp.concatenate(
                [qs[1, :, h * HEAD_DIM:(h + 1) * HEAD_DIM] for h in range(head * GROUP, (head + 1) * GROUP)], 0)
            for head in heads]
        scores = [dot_nt(keys_all[:, head_columns[head]], queries[head]) for head in heads]
        top = [jnp.max(scores[head], 0, keepdims=True) for head in heads]
        weights = [jnp.exp2((scores[head] - top[head]) * SCALE) for head in heads]
        return values_all, weights, [folded(weights[head]) for head in heads]

    def cross_add(weighed):
        values_all, weights, summed = weighed
        store(cout_v, [mix(values_all[:, head_columns[head]], weights[head]) for head in heads], summed)

    def image_start(item):
        send(2, item, 4, z != 1)
        send(2, item, 2)
        send(2, item, 6, z == 1)

    block([0], first=True)
    if paired:
        for part in range(2):
            take(part, 1)
        block([1])
        relay(0)
        relay(1)

        @pl.when(jnp.logical_and(core == 1, z == 3))
        def _():
            pl.semaphore_wait(ready.at[1], 1)
            send(2, 0, 6)
            take(2, 1)
            send(2, 1, 6)


        @on_core(1)
        def _():
            image_start(0)

        relay(2)

        @on_core(1)
        def _():
            pl.when(z != 3)(functools.partial(take, 2, 1))
            handed(1, 0).start()
            image_start(1)

        block(places)

        @on_core(1)
        def _():
            for item in range(2):
                send(2, item, 4, z == 1)

        @on_core(1)
        def _():
            for item in (4, 5):
                carry([item])
                send(2, item, 2, z % 2 == 0)

        for at in range(2):
            for part in range(2):
                take(part, places[at] + 1)
        block([places[0] + 1, places[1] + 1])

        rest = [places[2] + 1]

        @on_core(0)
        def _():
            for item in range(1, n):
                handed(item, 0).wait_recv()

        @on_core(1)
        def _():
            carry([2, 3, 6, 7])

        take(0, rest[0])
        weighed = weigh(rest)
        crossed = cross_weigh()
        take(1, rest[0])
        add(rest, weighed, last=True)
        cross_add(crossed)

        @on_core(0)
        def _():
            handed(0, 1).wait_send()

        @on_core(1)
        def _():
            landed(image.at[pl.ds(0, n - 1)], send_sem.at[1])
            landed(image.at[pl.ds(0, n - 1 - len(DIRECT)), 0], send_sem.at[2])
    else:
        for part in range(2):
            for mask, held in part_steps[part]:
                for item in held:
                    arrive_text(item ^ mask, part)
        for mask, held in image_steps:
            for item in held:
                arrive_image(item ^ mask)

        def step(item, unused):
            block([item])
            return 0

        lax.fori_loop(1, n, step, 0)
        store(out_v, [mixed[head] for head in heads], [total[head] for head in heads])
        cross_add(cross_weigh())
        landed(image.at[pl.ds(0, n - 1)], send_sem.at[1])
    landed(text.at[pl.ds(0, n - 1)], send_sem.at[0])


def flush(self_v, cross_v, self_hbm, cross_hbm, sems):
    copies = [
        pltpu.make_async_copy(self_v, self_hbm, sems.at[0]),
        pltpu.make_async_copy(cross_v, cross_hbm, sems.at[1]),
    ]
    for copy in copies:
        copy.start()
    for copy in copies:
        copy.wait()


def body(n, nx, cores, self_queries, self_keys, self_values, cross_queries, cross_keys, cross_values, span_order):
    rows, width = self_queries.shape
    kv_width = self_keys.shape[1]
    kv_local = kv_width // HEAD_DIM
    image_rows = cross_keys.shape[0]
    tables = rotary_tables(span_order.shape[0], rows // 2)
    anywhere = pl.BlockSpec(memory_space=pl.ANY)
    result = pltpu.VMEM((rows, width), jnp.bfloat16)
    held = pl.pallas_call(
        functools.partial(kernel, n, nx),
        out_shape=(result, result),
        in_specs=[anywhere] * 8,
        out_specs=(pl.BlockSpec(memory_space=pltpu.VMEM),) * 2,
        scratch_shapes=[
            pltpu.VMEM((n, 2, rows, kv_width), jnp.bfloat16),
            pltpu.VMEM((n, cores, 2, image_rows, kv_width), jnp.bfloat16),
            pltpu.VMEM((2, rows, width), jnp.bfloat16),
            pltpu.VMEM(tables.shape, jnp.float32),
            pltpu.VMEM((kv_local, GROUP * rows, HEAD_DIM), jnp.bfloat16),
            pltpu.VMEM((rows // 2, GROUP * rows), jnp.int32),
            pltpu.VMEM((kv_local, 1, GROUP * rows), jnp.float32),
            pltpu.VMEM((kv_local, 8, GROUP * rows), jnp.float32),
            pltpu.VMEM((kv_local, HEAD_DIM, GROUP * rows), jnp.float32),
            pltpu.SMEM(span_order.shape, jnp.int32),
            pltpu.SemaphoreType.DMA((5,)),
            pltpu.SemaphoreType.DMA((3,)),
            pltpu.SemaphoreType.DMA((n - 1, 2)),
            pltpu.SemaphoreType.DMA((n - 1,)),
            pltpu.SemaphoreType.DMA((1,)),
            pltpu.SemaphoreType.REGULAR((2,)),
        ],
        compiler_params=pltpu.CompilerParams(collective_id=0, has_side_effects=True),
    )(span_order, self_queries, self_keys, self_values, cross_queries, cross_keys, cross_values, tables)
    plain = jax.ShapeDtypeStruct((rows, width), jnp.bfloat16)
    return pl.pallas_call(
        flush,
        out_shape=(plain, plain),
        in_specs=[pl.BlockSpec(memory_space=pltpu.VMEM)] * 2,
        out_specs=(anywhere, anywhere),
        scratch_shapes=[pltpu.SemaphoreType.DMA((2,))],
    )(*[pltpu.with_memory_space_constraint(array, pltpu.VMEM) for array in held])


def fast_axis(mesh, n):
    line = mesh.devices[0, :, 0]
    coords = [getattr(device, "coords", None) for device in line]
    if any(c is None for c in coords):
        return 1
    nx = len({c[0] for c in coords})
    return nx if n % nx == 0 else 1


def solution(mesh):
    n = mesh.shape["context"]
    nx = fast_axis(mesh, n)
    cores = 2 if (n, nx, mesh.shape["tensor"]) == (8, 2, 2) else 1
    both = P(("groups", "context"), "tensor")
    return jax.shard_map(
        functools.partial(body, n, nx, cores), mesh=mesh,
        in_specs=(both,) * 6 + (P("groups"),), out_specs=(both, both), check_vma=False)
```

```python
import functools
import math

import jax
import jax.numpy as jnp
import numpy as np
from jax import lax
from jax.experimental import pallas as pl
from jax.experimental.pallas import tpu as pltpu
from jax.sharding import PartitionSpec as P

HEAD_DIM = 128
HEADS = 16
KV_HEADS = 4
GROUP = HEADS // KV_HEADS
NEG_FILL = -1e30
DIRECT = (2, 3, 6, 7)
SCALE = HEAD_DIM ** (-0.5) * math.log2(math.e)


def rotary_tables(spans, span_len):
    half = HEAD_DIM // 2
    frequency = 500000.0 ** (-(np.arange(half) * 2.0) / HEAD_DIM)
    frequency = np.concatenate([frequency, frequency])
    base = (np.arange(spans) * span_len)[:, None] * frequency[None, :]
    inner = np.arange(span_len)[:, None] * frequency[None, :]
    sign = np.where(np.arange(HEAD_DIM) < half, -1.0, 1.0)[None, :]
    inners = [np.cos(inner), np.sin(inner), np.cos(inner) * sign, np.sin(inner) * sign]
    return np.concatenate(inners + [np.cos(base), np.sin(base)]).astype(np.float32)


def doubling(order):
    held, steps = [0], []
    for mask in order:
        steps.append((mask, list(held)))
        held += [item ^ mask for item in held]
    return steps


def kernel(
    n, nx,
    order_hbm, q_hbm, k_hbm, v_hbm, cq_hbm, ck_hbm, cv_hbm, tables_hbm,
    out_v, cout_v,
    text, image, qs, tables, q_rot, gap, peak, total, mixed, order,
    load_sem, send_sem, text_recv, image_recv, mate_recv, ready,
):
    me = lax.axis_index("context")
    rows = qs.shape[1]
    span_len = rows // 2
    kv_local = text.shape[3] // HEAD_DIM
    image_rows = image.shape[3]
    paired = image.shape[1] == 2
    core = lax.axis_index("tensor") if paired else 0
    z, x = me // nx, me % nx

    x_masks = [1 << b for b in reversed(range(nx.bit_length() - 1))]
    z_masks = [nx << b for b in reversed(range((n // nx).bit_length() - 1))]
    masks = z_masks + x_masks
    z_x = doubling(z_masks + x_masks)
    z_x_z = doubling(z_masks[:1] + x_masks + z_masks[1:])
    x_z = doubling(x_masks + z_masks)
    part_steps = (z_x, z_x)
    image_steps = x_z

    def flipped(index, item):
        for mask in masks:
            bit = (item // mask) % 2
            index = index + mask * bit * (1 - 2 * ((index // mask) % 2))
        return index

    partner = {mask: flipped(me, mask) for mask in (range(1, n) if paired else masks)}

    barrier = pltpu.get_barrier_semaphore()

    def hail(sem, where):
        pl.semaphore_signal(sem, inc=1, device_id=where, device_id_type=pl.DeviceIdType.MESH)

    def greet():
        if not paired:
            for mask in masks:
                hail(barrier, {"context": partner[mask]})
            return
        hail(barrier, {"tensor": 1 - core})
        hail(barrier, {"context": partner[1]})
        hail(barrier, {"context": partner[2]})

        @pl.when(z == 0)
        def _():
            hail(barrier, {"context": me + 2 * nx})

        @pl.when(z == 1)
        def _():
            hail(barrier, {"context": me + nx})
            hail(barrier, {"context": me + 2 * nx})

        @pl.when(z == 2)
        def _():
            hail(barrier, {"context": me - nx})

    def meet():
        if not paired:
            pl.semaphore_wait(barrier, len(masks))
            return
        pl.semaphore_wait(barrier, 3 + jnp.where(z == 0, 0, jnp.where(z == 2, 2, 1)))

        @pl.when(z == 1)
        def _():
            hail(ready.at[0], {"context": me - nx})

        @pl.when(z == 2)
        def _():
            hail(ready.at[0], {"context": me - nx})
            hail(ready.at[0], {"context": me + nx})

        @pl.when(jnp.logical_and(z == 2, core == 0))
        def _():
            hail(ready.at[1], {"tensor": 1})

    greet()
    kv_loads = [
        pltpu.make_async_copy(k_hbm, text.at[0, 0], send_sem.at[0]),
        pltpu.make_async_copy(v_hbm, text.at[0, 1], send_sem.at[0]),
        pltpu.make_async_copy(ck_hbm, image.at[0, core, 0], send_sem.at[1]),
        pltpu.make_async_copy(cv_hbm, image.at[0, core, 1], send_sem.at[1]),
    ]
    other_loads = [
        pltpu.make_async_copy(order_hbm, order, load_sem.at[0]),
        pltpu.make_async_copy(tables_hbm, tables, load_sem.at[1]),
        pltpu.make_async_copy(q_hbm, qs.at[0], load_sem.at[2]),
        pltpu.make_async_copy(cq_hbm, qs.at[1], load_sem.at[2]),
    ]

    def landed(ref, sem):
        pltpu.make_async_copy(ref, ref, sem).wait()

    for load in kv_loads:
        load.start()
    for load in other_loads:
        load.start()
    landed(text.at[0], send_sem.at[0])
    landed(image.at[0, core], send_sem.at[1])
    meet()

    def text_sem(item, part):
        if not paired:
            return text_recv.at[item - 1, part]
        return text_recv.at[3, 0] if isinstance(item, int) and item == 1 else text_recv.at[item // 2 - 1, part]

    def image_sem(item):
        return image_recv.at[{1: 0, 4: 1, 5: 2}.get(item, 3) if paired else item - 1]

    def text_copy(item, part, mask):
        return pltpu.make_async_remote_copy(
            src_ref=text.at[item, part], dst_ref=text.at[item ^ mask, part],
            send_sem=send_sem.at[0], recv_sem=text_sem(item ^ mask, part),
            device_id={"context": partner[mask]}, device_id_type=pl.DeviceIdType.MESH)

    def image_copy(item, mask):
        return pltpu.make_async_remote_copy(
            src_ref=image.at[item], dst_ref=image.at[item ^ mask],
            send_sem=send_sem.at[1], recv_sem=image_sem(item ^ mask),
            device_id={"context": partner[mask]}, device_id_type=pl.DeviceIdType.MESH)

    def forward_text(item, part):
        for mask, held in part_steps[part]:
            if item in held:
                text_copy(item, part, mask).start()

    def forward_image(item):
        for mask, held in image_steps:
            if item in held:
                image_copy(item, mask).start()

    def arrive_text(item, part):
        text_copy(item ^ masks[0], part, masks[0]).wait_recv()
        forward_text(item, part)

    def arrive_image(item):
        image_copy(item ^ masks[0], masks[0]).wait_recv()
        forward_image(item)

    def send(kind, item, mask, cond=None):
        if kind == 2 and (item ^ mask) in DIRECT:
            copies = [straight(item, item ^ mask, half, partner[mask]) for half in range(2)]
        else:
            copies = [image_copy(item, mask) if kind == 2 else text_copy(item, kind, mask)]
        for copy in copies:
            if cond is None:
                copy.start()
            else:
                pl.when(cond)(copy.start)

    def straight(item, to, half, where):
        return pltpu.make_async_remote_copy(
            src_ref=image.at[item, half], dst_ref=image.at[to, half],
            send_sem=send_sem.at[1], recv_sem=image_sem(to),
            device_id={"context": where, "tensor": half}, device_id_type=pl.DeviceIdType.MESH)

    def pick(*values):
        result = values[-1]
        for at in range(len(values) - 2, -1, -1):
            result = jnp.where(z == at, values[at], result)
        return result

    def relayed(item, part, to, sem):
        return pltpu.make_async_remote_copy(
            src_ref=text.at[item, part], dst_ref=text.at[to, part], send_sem=send_sem.at[0], recv_sem=sem,
            device_id={"context": partner[1]}, device_id_type=pl.DeviceIdType.MESH)

    def relay(at):
        place, part = at // 2, at % 2
        item = places[place]
        if at == 3:
            item, part = jnp.where(z == 0, places[2], item), jnp.where(z == 0, 0, 1)
        if at == 4:
            item, part = jnp.where(z == 0, places[1], item), jnp.where(z == 0, 1, 0)
        relayed(item, part, item, text_sem(item, part)).wait_recv()
        relayed(item, part, item + 1, text_recv.at[4, part] if place else text_recv.at[3, 1]).start()
        if place < 2:
            send(at % 2, 4, 2, z == 2 * place)

    def both_in(item, column):
        landed(text.at[item], text_recv.at[3, column])

    def texts_in(part):
        landed(text.at[0], text_recv.at[4, part])

    def take(item):
        image_copy(item ^ 1, 1).wait_recv()

    def handed(item, where):
        return pltpu.make_async_remote_copy(
            src_ref=image.at[item, 0], dst_ref=image.at[item, 0],
            send_sem=send_sem.at[2], recv_sem=image_sem(item) if item else mate_recv.at[0],
            device_id={"tensor": where}, device_id_type=pl.DeviceIdType.MESH)

    def carry(items):
        for item in items:
            take(item)
            handed(item, 0).start()

    def on_core(which):
        return pl.when(core == which)

    if paired:
        places = [pick(4, 2, 6, 2), pick(6, 4, 4, 4), pick(2, 6, 2, 6)]
        for part in range(2):
            send(part, 0, 1)
            send(part, 0, 2, z != 3)
            send(part, 0, 6, z == 1)
            send(part, 0, 4, z == 2)
        on_core(0)(handed(0, 1).start)

        @pl.when(z != 2)
        def _():
            pl.semaphore_wait(ready.at[0], 1)

        for mask, cond in ((6, z == 3), (2, z == 3), (4, z != 2)):
            for part in range(2):
                send(part, 0, mask, cond)

        @on_core(1)
        def _():
            handed(0, 0).wait_recv()
            send(2, 0, 1)

            @pl.when(z == 2)
            def _():
                pl.semaphore_wait(ready.at[1], 1)
                hail(ready.at[1], {"context": me + nx})
    else:
        forward_text(0, 0)
        forward_text(0, 1)
        forward_image(0)

    other_loads[0].wait()
    other_loads[1].wait()
    landed(qs, load_sem.at[2])

    spans = order.shape[0]

    def angles(place):
        inners = [tables[at * span_len:(at + 1) * span_len, :] for at in range(4)]
        cosines, sines, starts = [], [], []
        for part in range(2):
            span = order[2 * place + part]
            base_cos = tables[pl.ds(4 * span_len + span, 1), :]
            base_sin = tables[pl.ds(4 * span_len + spans + span, 1), :]
            cosines.append(base_cos * inners[0] - base_sin * inners[1])
            sines.append(base_sin * inners[2] + base_cos * inners[3])
            starts.append(span * span_len)
        return jnp.concatenate(cosines, 0), jnp.concatenate(sines, 0), starts

    def rotate(values, cosine, sine):
        values = values.astype(jnp.float32)
        turned = pltpu.roll(values, HEAD_DIM // 2, 1)
        return (values * cosine + turned * sine).astype(jnp.bfloat16)

    own_cos, own_sin, own_starts = angles(me)
    lane = lax.broadcasted_iota(jnp.int32, gap.shape, 1)
    for g in range(1, GROUP):
        lane = jnp.where(lane >= rows, lane - rows, lane)
    own_places = jnp.where(lane < span_len, own_starts[0] + lane, own_starts[1] + lane - span_len)
    gap[...] = own_places - lax.broadcasted_iota(jnp.int32, gap.shape, 0)
    for head in range(kv_local * GROUP):
        q_rot[head // GROUP, pl.ds(head % GROUP * rows, rows), :] = rotate(
            qs[0, :, head * HEAD_DIM:(head + 1) * HEAD_DIM], own_cos, own_sin)

    def dot_nt(a, b):
        return lax.dot_general(a, b, (((1,), (1,)), ((), ())), preferred_element_type=jnp.float32)

    def join(pieces):
        return pieces[0] if len(pieces) == 1 else jnp.concatenate(pieces, 0)

    def mix(values, weights):
        return lax.dot_general(
            values, weights.astype(jnp.bfloat16), (((0,), (0,)), ((), ())), preferred_element_type=jnp.float32)

    def folded(weights):
        return jnp.sum(weights.reshape(-1, 8, weights.shape[1]), 0)

    heads = range(kv_local)
    head_columns = [slice(head * HEAD_DIM, (head + 1) * HEAD_DIM) for head in heads]

    def weigh(items, first=False):
        parts = [angles(flipped(me, item)) for item in items]
        cosine, sine = join([p[0] for p in parts]), join([p[1] for p in parts])
        starts = sum([p[2] for p in parts], [])
        keys = [rotate(join([text[item, 0, :, at] for item in items]), cosine, sine) for at in head_columns]
        scores = [dot_nt(keys[head], q_rot[head]) for head in heads]
        scores = [join([
            jnp.where(gap[...] >= starts[at], block_scores[at * span_len:(at + 1) * span_len], NEG_FILL)
            for at in range(len(starts))]) for block_scores in scores]
        top = [jnp.max(block_scores, 0, keepdims=True) for block_scores in scores]
        if not first:
            old = [peak[head] for head in heads]
            top = [jnp.maximum(top[head], old[head]) for head in heads]
        weights = [jnp.exp2((scores[head] - top[head]) * SCALE) for head in heads]
        summed = [folded(weights[head]) for head in heads]
        if first:
            return top, weights, summed, None
        factor = [jnp.exp2((old[head] - top[head]) * SCALE) for head in heads]
        return top, weights, [summed[head] + total[head] * factor[head] for head in heads], factor

    def add(items, weighed, last=False):
        top, weights, summed, factor = weighed
        values = [join([text[item, 1, :, at] for item in items]) for at in head_columns]
        product = [mix(values[head], weights[head]) for head in heads]
        if factor is not None:
            product = [product[head] + mixed[head] * factor[head] for head in heads]
        if last:
            store(out_v, product, summed)
            return
        for head in heads:
            peak[head] = top[head]
            total[head] = summed[head]
            mixed[head] = product[head]

    def block(items, first=False):
        add(items, weigh(items, first))

    def store(target, product, summed):
        result = [
            (product[head] * (1.0 / jnp.sum(summed[head], 0, keepdims=True))).T.astype(jnp.bfloat16) for head in heads]
        for head in heads:
            for g in range(GROUP):
                at = head * GROUP + g
                target[:, at * HEAD_DIM:(at + 1) * HEAD_DIM] = result[head][g * rows:(g + 1) * rows]

    def cross_weigh():
        keys_all = image[:, core, 0].astype(jnp.float32).reshape(n * image_rows, -1).astype(jnp.bfloat16)
        values_all = image[:, core, 1].astype(jnp.float32).reshape(n * image_rows, -1).astype(jnp.bfloat16)
        queries = [
            jnp.concatenate(
                [qs[1, :, h * HEAD_DIM:(h + 1) * HEAD_DIM] for h in range(head * GROUP, (head + 1) * GROUP)], 0)
            for head in heads]
        scores = [dot_nt(keys_all[:, head_columns[head]], queries[head]) for head in heads]
        top = [jnp.max(scores[head], 0, keepdims=True) for head in heads]
        weights = [jnp.exp2((scores[head] - top[head]) * SCALE) for head in heads]
        return values_all, weights, [folded(weights[head]) for head in heads]

    def cross_add(weighed):
        values_all, weights, summed = weighed
        store(cout_v, [mix(values_all[:, head_columns[head]], weights[head]) for head in heads], summed)

    def image_start(item):
        send(2, item, 4, z != 1)
        send(2, item, 2)
        send(2, item, 6, z == 1)

    block([0], first=True)
    if paired:
        both_in(1, 0)
        block([1])
        relay(0)
        relay(1)
        relay(2)
        relay(3)

        @pl.when(jnp.logical_and(core == 1, z == 3))
        def _():
            pl.semaphore_wait(ready.at[1], 1)
            send(2, 0, 6)
            take(1)
            send(2, 1, 6)


        @on_core(1)
        def _():
            image_start(0)

        relay(4)
        relay(5)

        @on_core(1)
        def _():
            pl.when(z != 3)(functools.partial(take, 1))
            handed(1, 0).start()
            image_start(1)

        block(places)

        @on_core(1)
        def _():
            for item in range(2):
                send(2, item, 4, z == 1)

        rest = [place + 1 for place in places]

        @on_core(0)
        def _():
            both_in(rest[0], 1)
            block(rest[:1])
            texts_in(0)
            weighed = weigh(rest[1:])
            for item in (1, 4, 5):
                handed(item, 0).wait_recv()
            landed(image.at[pl.ds(0, len(DIRECT)), 0], image_sem(DIRECT[0]))
            crossed = cross_weigh()
            texts_in(1)
            add(rest[1:], weighed, last=True)
            cross_add(crossed)

        @on_core(1)
        def _():
            carry([4])
            send(2, 4, 2, z % 2 == 0)
            both_in(rest[0], 1)
            for part in range(2):
                texts_in(part)
            add(rest, weigh(rest), last=True)
            carry([5])
            send(2, 5, 2, z % 2 == 0)
            landed(image.at[pl.ds(0, len(DIRECT)), 1], image_sem(DIRECT[0]))
            cross_add(cross_weigh())

        @on_core(0)
        def _():
            handed(0, 1).wait_send()

        @on_core(1)
        def _():
            landed(image.at[pl.ds(0, n - 1)], send_sem.at[1])
            landed(image.at[pl.ds(0, n - 1 - len(DIRECT)), 0], send_sem.at[2])
    else:
        for part in range(2):
            for mask, held in part_steps[part]:
                for item in held:
                    arrive_text(item ^ mask, part)
        for mask, held in image_steps:
            for item in held:
                arrive_image(item ^ mask)

        def step(item, unused):
            block([item])
            return 0

        lax.fori_loop(1, n, step, 0)
        store(out_v, [mixed[head] for head in heads], [total[head] for head in heads])
        cross_add(cross_weigh())
        landed(image.at[pl.ds(0, n - 1)], send_sem.at[1])
    landed(text.at[pl.ds(0, n - 1)], send_sem.at[0])


def flush(self_v, cross_v, self_hbm, cross_hbm, sems):
    copies = [
        pltpu.make_async_copy(self_v, self_hbm, sems.at[0]),
        pltpu.make_async_copy(cross_v, cross_hbm, sems.at[1]),
    ]
    for copy in copies:
        copy.start()
    for copy in copies:
        copy.wait()


def body(n, nx, cores, self_queries, self_keys, self_values, cross_queries, cross_keys, cross_values, span_order):
    rows, width = self_queries.shape
    kv_width = self_keys.shape[1]
    kv_local = kv_width // HEAD_DIM
    image_rows = cross_keys.shape[0]
    tables = rotary_tables(span_order.shape[0], rows // 2)
    anywhere = pl.BlockSpec(memory_space=pl.ANY)
    result = pltpu.VMEM((rows, width), jnp.bfloat16)
    held = pl.pallas_call(
        functools.partial(kernel, n, nx),
        out_shape=(result, result),
        in_specs=[anywhere] * 8,
        out_specs=(pl.BlockSpec(memory_space=pltpu.VMEM),) * 2,
        scratch_shapes=[
            pltpu.VMEM((n, 2, rows, kv_width), jnp.bfloat16),
            pltpu.VMEM((n, cores, 2, image_rows, kv_width), jnp.bfloat16),
            pltpu.VMEM((2, rows, width), jnp.bfloat16),
            pltpu.VMEM(tables.shape, jnp.float32),
            pltpu.VMEM((kv_local, GROUP * rows, HEAD_DIM), jnp.bfloat16),
            pltpu.VMEM((rows // 2, GROUP * rows), jnp.int32),
            pltpu.VMEM((kv_local, 1, GROUP * rows), jnp.float32),
            pltpu.VMEM((kv_local, 8, GROUP * rows), jnp.float32),
            pltpu.VMEM((kv_local, HEAD_DIM, GROUP * rows), jnp.float32),
            pltpu.SMEM(span_order.shape, jnp.int32),
            pltpu.SemaphoreType.DMA((3,)),
            pltpu.SemaphoreType.DMA((3,)),
            pltpu.SemaphoreType.DMA((5 if cores == 2 else n - 1, 2)),
            pltpu.SemaphoreType.DMA((4 if cores == 2 else n - 1,)),
            pltpu.SemaphoreType.DMA((1,)),
            pltpu.SemaphoreType.REGULAR((2,)),
        ],
        compiler_params=pltpu.CompilerParams(collective_id=0, has_side_effects=True),
    )(span_order, self_queries, self_keys, self_values, cross_queries, cross_keys, cross_values, tables)
    plain = jax.ShapeDtypeStruct((rows, width), jnp.bfloat16)
    return pl.pallas_call(
        flush,
        out_shape=(plain, plain),
        in_specs=[pl.BlockSpec(memory_space=pltpu.VMEM)] * 2,
        out_specs=(anywhere, anywhere),
        scratch_shapes=[pltpu.SemaphoreType.DMA((2,))],
    )(*[pltpu.with_memory_space_constraint(array, pltpu.VMEM) for array in held])


def fast_axis(mesh, n):
    line = mesh.devices[0, :, 0]
    coords = [getattr(device, "coords", None) for device in line]
    if any(c is None for c in coords):
        return 1
    nx = len({c[0] for c in coords})
    return nx if n % nx == 0 else 1


def solution(mesh):
    n = mesh.shape["context"]
    nx = fast_axis(mesh, n)
    cores = 2 if (n, nx, mesh.shape["tensor"]) == (8, 2, 2) else 1
    both = P(("groups", "context"), "tensor")
    return jax.shard_map(
        functools.partial(body, n, nx, cores), mesh=mesh,
        in_specs=(both,) * 6 + (P("groups"),), out_specs=(both, both), check_vma=False)
```

```python
import functools
import math

import jax
import jax.numpy as jnp
import numpy as np
from jax import lax
from jax.experimental import pallas as pl
from jax.experimental.pallas import tpu as pltpu
from jax.sharding import PartitionSpec as P

HEAD_DIM = 128
HEADS = 16
KV_HEADS = 4
GROUP = HEADS // KV_HEADS
NEG_FILL = -1e30
DIRECT = (2, 3, 6, 7)
SCALE = HEAD_DIM ** (-0.5) * math.log2(math.e)


def rotary_tables(spans, span_len):
    half = HEAD_DIM // 2
    frequency = 500000.0 ** (-(np.arange(half) * 2.0) / HEAD_DIM)
    frequency = np.concatenate([frequency, frequency])
    base = (np.arange(spans) * span_len)[:, None] * frequency[None, :]
    inner = np.arange(span_len)[:, None] * frequency[None, :]
    sign = np.where(np.arange(HEAD_DIM) < half, -1.0, 1.0)[None, :]
    inners = [np.cos(inner), np.sin(inner), np.cos(inner) * sign, np.sin(inner) * sign]
    return np.concatenate(inners + [np.cos(base), np.sin(base)]).astype(np.float32)


def doubling(order):
    held, steps = [0], []
    for mask in order:
        steps.append((mask, list(held)))
        held += [item ^ mask for item in held]
    return steps


def kernel(
    n, nx,
    order_hbm, q_hbm, k_hbm, v_hbm, cq_hbm, ck_hbm, cv_hbm, tables_hbm,
    out_v, cout_v,
    text, image, qs, tables, q_rot, gap, peak, total, mixed, order,
    load_sem, send_sem, text_recv, image_recv, mate_recv, ready,
):
    me = lax.axis_index("context")
    rows = qs.shape[1]
    span_len = rows // 2
    kv_local = text.shape[3] // HEAD_DIM
    image_rows = image.shape[3]
    paired = image.shape[1] == 2
    core = lax.axis_index("tensor") if paired else 0
    z, x = me // nx, me % nx

    x_masks = [1 << b for b in reversed(range(nx.bit_length() - 1))]
    z_masks = [nx << b for b in reversed(range((n // nx).bit_length() - 1))]
    masks = z_masks + x_masks
    z_x = doubling(z_masks + x_masks)
    z_x_z = doubling(z_masks[:1] + x_masks + z_masks[1:])
    x_z = doubling(x_masks + z_masks)
    part_steps = (z_x, z_x)
    image_steps = x_z

    def flipped(index, item):
        for mask in masks:
            bit = (item // mask) % 2
            index = index + mask * bit * (1 - 2 * ((index // mask) % 2))
        return index

    partner = {mask: flipped(me, mask) for mask in (range(1, n) if paired else masks)}

    barrier = pltpu.get_barrier_semaphore()

    def hail(sem, where):
        pl.semaphore_signal(sem, inc=1, device_id=where, device_id_type=pl.DeviceIdType.MESH)

    def greet():
        if not paired:
            for mask in masks:
                hail(barrier, {"context": partner[mask]})
            return
        hail(barrier, {"tensor": 1 - core})
        hail(barrier, {"context": partner[1]})
        hail(barrier, {"context": partner[2]})

        @pl.when(z == 0)
        def _():
            hail(barrier, {"context": me + 2 * nx})

        @pl.when(z == 1)
        def _():
            hail(barrier, {"context": me + nx})
            hail(barrier, {"context": me + 2 * nx})

        @pl.when(z == 2)
        def _():
            hail(barrier, {"context": me - nx})

    def meet():
        if not paired:
            pl.semaphore_wait(barrier, len(masks))
            return
        pl.semaphore_wait(barrier, 3 + jnp.where(z == 0, 0, jnp.where(z == 2, 2, 1)))

        @pl.when(z == 1)
        def _():
            hail(ready.at[0], {"context": me - nx})

        @pl.when(z == 2)
        def _():
            hail(ready.at[0], {"context": me - nx})
            hail(ready.at[0], {"context": me + nx})

        @pl.when(jnp.logical_and(z == 2, core == 0))
        def _():
            hail(ready.at[1], {"tensor": 1})

    greet()
    kv_loads = [
        pltpu.make_async_copy(k_hbm, text.at[0, 0], send_sem.at[0]),
        pltpu.make_async_copy(v_hbm, text.at[0, 1], send_sem.at[0]),
        pltpu.make_async_copy(ck_hbm, image.at[0, core, 0], send_sem.at[1]),
        pltpu.make_async_copy(cv_hbm, image.at[0, core, 1], send_sem.at[1]),
    ]
    other_loads = [
        pltpu.make_async_copy(order_hbm, order, load_sem.at[0]),
        pltpu.make_async_copy(tables_hbm, tables, load_sem.at[1]),
        pltpu.make_async_copy(q_hbm, qs.at[0], load_sem.at[2]),
        pltpu.make_async_copy(cq_hbm, qs.at[1], load_sem.at[2]),
    ]

    def landed(ref, sem):
        pltpu.make_async_copy(ref, ref, sem).wait()

    for load in kv_loads:
        load.start()
    for load in other_loads:
        load.start()
    landed(text.at[0], send_sem.at[0])
    landed(image.at[0, core], send_sem.at[1])
    meet()

    def text_sem(item, part):
        if not paired:
            return text_recv.at[item - 1, part]
        return text_recv.at[3, 0] if isinstance(item, int) and item == 1 else text_recv.at[item // 2 - 1, part]

    def image_sem(item):
        return image_recv.at[{1: 0, 4: 1, 5: 2}.get(item, 3) if paired else item - 1]

    def text_copy(item, part, mask):
        return pltpu.make_async_remote_copy(
            src_ref=text.at[item, part], dst_ref=text.at[item ^ mask, part],
            send_sem=send_sem.at[0], recv_sem=text_sem(item ^ mask, part),
            device_id={"context": partner[mask]}, device_id_type=pl.DeviceIdType.MESH)

    def image_copy(item, mask):
        return pltpu.make_async_remote_copy(
            src_ref=image.at[item], dst_ref=image.at[item ^ mask],
            send_sem=send_sem.at[1], recv_sem=image_sem(item ^ mask),
            device_id={"context": partner[mask]}, device_id_type=pl.DeviceIdType.MESH)

    def forward_text(item, part):
        for mask, held in part_steps[part]:
            if item in held:
                text_copy(item, part, mask).start()

    def forward_image(item):
        for mask, held in image_steps:
            if item in held:
                image_copy(item, mask).start()

    def arrive_text(item, part):
        text_copy(item ^ masks[0], part, masks[0]).wait_recv()
        forward_text(item, part)

    def arrive_image(item):
        image_copy(item ^ masks[0], masks[0]).wait_recv()
        forward_image(item)

    def send(kind, item, mask, cond=None, whole=None):
        if kind == 2 and (whole is False or whole is None and (item ^ mask) in DIRECT):
            copies = [straight(item, item ^ mask, half, partner[mask]) for half in range(2)]
        else:
            copies = [image_copy(item, mask) if kind == 2 else text_copy(item, kind, mask)]
        for copy in copies:
            if cond is None:
                copy.start()
            else:
                pl.when(cond)(copy.start)

    def straight(item, to, half, where):
        return pltpu.make_async_remote_copy(
            src_ref=image.at[item, half], dst_ref=image.at[to, half],
            send_sem=send_sem.at[1], recv_sem=image_sem(to),
            device_id={"context": where, "tensor": half}, device_id_type=pl.DeviceIdType.MESH)

    def pick(*values):
        result = values[-1]
        for at in range(len(values) - 2, -1, -1):
            result = jnp.where(z == at, values[at], result)
        return result

    def relayed(item, part, to, sem):
        return pltpu.make_async_remote_copy(
            src_ref=text.at[item, part], dst_ref=text.at[to, part], send_sem=send_sem.at[0], recv_sem=sem,
            device_id={"context": partner[1]}, device_id_type=pl.DeviceIdType.MESH)

    def relay(at):
        place, part = at // 2, at % 2
        item = places[place]
        if at == 3:
            item, part = jnp.where(z == 0, places[2], item), jnp.where(z == 0, 0, 1)
        if at == 4:
            item, part = jnp.where(z == 0, places[1], item), jnp.where(z == 0, 1, 0)
        relayed(item, part, item, text_sem(item, part)).wait_recv()
        relayed(item, part, item + 1, text_recv.at[4, part] if place else text_recv.at[3, 1]).start()
        if place < 2:
            send(at % 2, 4, 2, z == 2 * place)

    def both_in(item, column):
        landed(text.at[item], text_recv.at[3, column])

    def texts_in(part):
        landed(text.at[0], text_recv.at[4, part])

    def take(item):
        image_copy(item ^ 1, 1).wait_recv()

    def handed(item, where):
        return pltpu.make_async_remote_copy(
            src_ref=image.at[item, 0], dst_ref=image.at[item, 0],
            send_sem=send_sem.at[2], recv_sem=image_sem(item) if item else mate_recv.at[0],
            device_id={"tensor": where}, device_id_type=pl.DeviceIdType.MESH)

    def carry(items):
        for item in items:
            take(item)
            handed(item, 0).start()

    def forward(item):
        @pl.when(z % 2 == 0)
        def _():
            carry([item])
            send(2, item, 2)

        @pl.when(z % 2 == 1)
        def _():
            straight(item, item, 1, partner[1]).wait_recv()

    def on_core(which):
        return pl.when(core == which)

    if paired:
        places = [pick(4, 2, 6, 2), pick(6, 4, 4, 4), pick(2, 6, 2, 6)]
        for part in range(2):
            send(part, 0, 1)
            send(part, 0, 2, z != 3)
            send(part, 0, 6, z == 1)
            send(part, 0, 4, z == 2)
        on_core(0)(handed(0, 1).start)

        @pl.when(z != 2)
        def _():
            pl.semaphore_wait(ready.at[0], 1)

        for mask, cond in ((6, z == 3), (2, z == 3), (4, z != 2)):
            for part in range(2):
                send(part, 0, mask, cond)

        @on_core(1)
        def _():
            handed(0, 0).wait_recv()
            send(2, 0, 1)

            @pl.when(z == 2)
            def _():
                pl.semaphore_wait(ready.at[1], 1)
                hail(ready.at[1], {"context": me + nx})
    else:
        forward_text(0, 0)
        forward_text(0, 1)
        forward_image(0)

    other_loads[0].wait()
    other_loads[1].wait()
    landed(qs, load_sem.at[2])

    spans = order.shape[0]

    def angles(place):
        inners = [tables[at * span_len:(at + 1) * span_len, :] for at in range(4)]
        cosines, sines, starts = [], [], []
        for part in range(2):
            span = order[2 * place + part]
            base_cos = tables[pl.ds(4 * span_len + span, 1), :]
            base_sin = tables[pl.ds(4 * span_len + spans + span, 1), :]
            cosines.append(base_cos * inners[0] - base_sin * inners[1])
            sines.append(base_sin * inners[2] + base_cos * inners[3])
            starts.append(span * span_len)
        return jnp.concatenate(cosines, 0), jnp.concatenate(sines, 0), starts

    def rotate(values, cosine, sine):
        values = values.astype(jnp.float32)
        turned = pltpu.roll(values, HEAD_DIM // 2, 1)
        return (values * cosine + turned * sine).astype(jnp.bfloat16)

    own_cos, own_sin, own_starts = angles(me)
    lane = lax.broadcasted_iota(jnp.int32, gap.shape, 1)
    for g in range(1, GROUP):
        lane = jnp.where(lane >= rows, lane - rows, lane)
    own_places = jnp.where(lane < span_len, own_starts[0] + lane, own_starts[1] + lane - span_len)
    gap[...] = own_places - lax.broadcasted_iota(jnp.int32, gap.shape, 0)
    for head in range(kv_local * GROUP):
        q_rot[head // GROUP, pl.ds(head % GROUP * rows, rows), :] = rotate(
            qs[0, :, head * HEAD_DIM:(head + 1) * HEAD_DIM], own_cos, own_sin)

    def dot_nt(a, b):
        return lax.dot_general(a, b, (((1,), (1,)), ((), ())), preferred_element_type=jnp.float32)

    def join(pieces):
        return pieces[0] if len(pieces) == 1 else jnp.concatenate(pieces, 0)

    def mix(values, weights):
        return lax.dot_general(
            values, weights.astype(jnp.bfloat16), (((0,), (0,)), ((), ())), preferred_element_type=jnp.float32)

    def folded(weights):
        return jnp.sum(weights.reshape(-1, 8, weights.shape[1]), 0)

    heads = range(kv_local)
    head_columns = [slice(head * HEAD_DIM, (head + 1) * HEAD_DIM) for head in heads]

    def weigh(items, first=False):
        parts = [angles(flipped(me, item)) for item in items]
        cosine, sine = join([p[0] for p in parts]), join([p[1] for p in parts])
        starts = sum([p[2] for p in parts], [])
        keys = [rotate(join([text[item, 0, :, at] for item in items]), cosine, sine) for at in head_columns]
        scores = [dot_nt(keys[head], q_rot[head]) for head in heads]
        scores = [join([
            jnp.where(gap[...] >= starts[at], block_scores[at * span_len:(at + 1) * span_len], NEG_FILL)
            for at in range(len(starts))]) for block_scores in scores]
        top = [jnp.max(block_scores, 0, keepdims=True) for block_scores in scores]
        if not first:
            old = [peak[head] for head in heads]
            top = [jnp.maximum(top[head], old[head]) for head in heads]
        weights = [jnp.exp2((scores[head] - top[head]) * SCALE) for head in heads]
        summed = [folded(weights[head]) for head in heads]
        if first:
            return top, weights, summed, None
        factor = [jnp.exp2((old[head] - top[head]) * SCALE) for head in heads]
        return top, weights, [summed[head] + total[head] * factor[head] for head in heads], factor

    def add(items, weighed, last=False):
        top, weights, summed, factor = weighed
        values = [join([text[item, 1, :, at] for item in items]) for at in head_columns]
        product = [mix(values[head], weights[head]) for head in heads]
        if factor is not None:
            product = [product[head] + mixed[head] * factor[head] for head in heads]
        if last:
            store(out_v, product, summed)
            return
        for head in heads:
            peak[head] = top[head]
            total[head] = summed[head]
            mixed[head] = product[head]

    def block(items, first=False):
        add(items, weigh(items, first))

    def store(target, product, summed):
        result = [
            (product[head] * (1.0 / jnp.sum(summed[head], 0, keepdims=True))).T.astype(jnp.bfloat16) for head in heads]
        for head in heads:
            for g in range(GROUP):
                at = head * GROUP + g
                target[:, at * HEAD_DIM:(at + 1) * HEAD_DIM] = result[head][g * rows:(g + 1) * rows]

    def cross_weigh():
        keys_all = image[:, core, 0].astype(jnp.float32).reshape(n * image_rows, -1).astype(jnp.bfloat16)
        values_all = image[:, core, 1].astype(jnp.float32).reshape(n * image_rows, -1).astype(jnp.bfloat16)
        queries = [
            jnp.concatenate(
                [qs[1, :, h * HEAD_DIM:(h + 1) * HEAD_DIM] for h in range(head * GROUP, (head + 1) * GROUP)], 0)
            for head in heads]
        scores = [dot_nt(keys_all[:, head_columns[head]], queries[head]) for head in heads]
        top = [jnp.max(scores[head], 0, keepdims=True) for head in heads]
        weights = [jnp.exp2((scores[head] - top[head]) * SCALE) for head in heads]
        return values_all, weights, [folded(weights[head]) for head in heads]

    def cross_add(weighed):
        values_all, weights, summed = weighed
        store(cout_v, [mix(values_all[:, head_columns[head]], weights[head]) for head in heads], summed)

    def image_start(item):
        send(2, item, 4, z % 2 == 0)
        send(2, item, 4, z == 3, whole=False)
        send(2, item, 2)
        send(2, item, 6, z == 1)

    block([0], first=True)
    if paired:
        both_in(1, 0)
        block([1])
        relay(0)
        relay(1)
        relay(2)
        relay(3)

        @pl.when(jnp.logical_and(core == 1, z == 3))
        def _():
            pl.semaphore_wait(ready.at[1], 1)
            send(2, 0, 6)
            take(1)
            send(2, 1, 6)


        @on_core(1)
        def _():
            image_start(0)

        relay(4)
        relay(5)

        @on_core(1)
        def _():
            pl.when(z != 3)(functools.partial(take, 1))
            handed(1, 0).start()
            image_start(1)

        block(places)

        @on_core(1)
        def _():
            for item in range(2):
                send(2, item, 4, z == 1, whole=False)

        rest = [place + 1 for place in places]

        def images_in():
            for item in (1, 4, 5):
                handed(item, 0).wait_recv()
            landed(image.at[pl.ds(0, len(DIRECT)), 0], image_sem(DIRECT[0]))

        @on_core(0)
        def _():
            both_in(rest[0], 1)
            block(rest[:1])

            @pl.when(z > 0)
            def _():
                images_in()
                cross_add(cross_weigh())

            texts_in(0)
            weighed = weigh(rest[1:])

            @pl.when(z == 0)
            def _():
                images_in()
                crossed = cross_weigh()
                texts_in(1)
                add(rest[1:], weighed, last=True)
                cross_add(crossed)

            @pl.when(z > 0)
            def _():
                texts_in(1)
                add(rest[1:], weighed, last=True)

        @on_core(1)
        def _():
            forward(4)
            both_in(rest[0], 1)
            for part in range(2):
                texts_in(part)
            add(rest, weigh(rest), last=True)
            forward(5)
            landed(image.at[pl.ds(0, len(DIRECT)), 1], image_sem(DIRECT[0]))
            cross_add(cross_weigh())

        @on_core(0)
        def _():
            handed(0, 1).wait_send()

        @on_core(1)
        def _():
            landed(image.at[pl.ds(0, n - 1)], send_sem.at[1])
            handed(1, 0).wait_send()

            @pl.when(z % 2 == 0)
            def _():
                landed(image.at[pl.ds(0, 2), 0], send_sem.at[2])
    else:
        for part in range(2):
            for mask, held in part_steps[part]:
                for item in held:
                    arrive_text(item ^ mask, part)
        for mask, held in image_steps:
            for item in held:
                arrive_image(item ^ mask)

        def step(item, unused):
            block([item])
            return 0

        lax.fori_loop(1, n, step, 0)
        store(out_v, [mixed[head] for head in heads], [total[head] for head in heads])
        cross_add(cross_weigh())
        landed(image.at[pl.ds(0, n - 1)], send_sem.at[1])
    landed(text.at[pl.ds(0, n - 1)], send_sem.at[0])


def flush(self_v, cross_v, self_hbm, cross_hbm, sems):
    copies = [
        pltpu.make_async_copy(self_v, self_hbm, sems.at[0]),
        pltpu.make_async_copy(cross_v, cross_hbm, sems.at[1]),
    ]
    for copy in copies:
        copy.start()
    for copy in copies:
        copy.wait()


def body(n, nx, cores, self_queries, self_keys, self_values, cross_queries, cross_keys, cross_values, span_order):
    rows, width = self_queries.shape
    kv_width = self_keys.shape[1]
    kv_local = kv_width // HEAD_DIM
    image_rows = cross_keys.shape[0]
    tables = rotary_tables(span_order.shape[0], rows // 2)
    anywhere = pl.BlockSpec(memory_space=pl.ANY)
    result = pltpu.VMEM((rows, width), jnp.bfloat16)
    held = pl.pallas_call(
        functools.partial(kernel, n, nx),
        out_shape=(result, result),
        in_specs=[anywhere] * 8,
        out_specs=(pl.BlockSpec(memory_space=pltpu.VMEM),) * 2,
        scratch_shapes=[
            pltpu.VMEM((n, 2, rows, kv_width), jnp.bfloat16),
            pltpu.VMEM((n, cores, 2, image_rows, kv_width), jnp.bfloat16),
            pltpu.VMEM((2, rows, width), jnp.bfloat16),
            pltpu.VMEM(tables.shape, jnp.float32),
            pltpu.VMEM((kv_local, GROUP * rows, HEAD_DIM), jnp.bfloat16),
            pltpu.VMEM((rows // 2, GROUP * rows), jnp.int32),
            pltpu.VMEM((kv_local, 1, GROUP * rows), jnp.float32),
            pltpu.VMEM((kv_local, 8, GROUP * rows), jnp.float32),
            pltpu.VMEM((kv_local, HEAD_DIM, GROUP * rows), jnp.float32),
            pltpu.SMEM(span_order.shape, jnp.int32),
            pltpu.SemaphoreType.DMA((3,)),
            pltpu.SemaphoreType.DMA((3,)),
            pltpu.SemaphoreType.DMA((5 if cores == 2 else n - 1, 2)),
            pltpu.SemaphoreType.DMA((4 if cores == 2 else n - 1,)),
            pltpu.SemaphoreType.DMA((1,)),
            pltpu.SemaphoreType.REGULAR((2,)),
        ],
        compiler_params=pltpu.CompilerParams(collective_id=0, has_side_effects=True),
    )(span_order, self_queries, self_keys, self_values, cross_queries, cross_keys, cross_values, tables)
    plain = jax.ShapeDtypeStruct((rows, width), jnp.bfloat16)
    return pl.pallas_call(
        flush,
        out_shape=(plain, plain),
        in_specs=[pl.BlockSpec(memory_space=pltpu.VMEM)] * 2,
        out_specs=(anywhere, anywhere),
        scratch_shapes=[pltpu.SemaphoreType.DMA((2,))],
    )(*[pltpu.with_memory_space_constraint(array, pltpu.VMEM) for array in held])


def fast_axis(mesh, n):
    line = mesh.devices[0, :, 0]
    coords = [getattr(device, "coords", None) for device in line]
    if any(c is None for c in coords):
        return 1
    nx = len({c[0] for c in coords})
    return nx if n % nx == 0 else 1


def solution(mesh):
    n = mesh.shape["context"]
    nx = fast_axis(mesh, n)
    cores = 2 if (n, nx, mesh.shape["tensor"]) == (8, 2, 2) else 1
    both = P(("groups", "context"), "tensor")
    return jax.shard_map(
        functools.partial(body, n, nx, cores), mesh=mesh,
        in_specs=(both,) * 6 + (P("groups"),), out_specs=(both, both), check_vma=False)
```

```python
import functools
import math

import jax
import jax.numpy as jnp
import numpy as np
from jax import lax
from jax.experimental import pallas as pl
from jax.experimental.pallas import tpu as pltpu
from jax.sharding import PartitionSpec as P

HEAD_DIM = 128
HEADS = 16
KV_HEADS = 4
GROUP = HEADS // KV_HEADS
NEG_FILL = -1e30
DIRECT = (2, 3, 6, 7)
SCALE = HEAD_DIM ** (-0.5) * math.log2(math.e)


def rotary_tables(spans, span_len):
    half = HEAD_DIM // 2
    frequency = 500000.0 ** (-(np.arange(half) * 2.0) / HEAD_DIM)
    frequency = np.concatenate([frequency, frequency])
    base = (np.arange(spans) * span_len)[:, None] * frequency[None, :]
    inner = np.arange(span_len)[:, None] * frequency[None, :]
    sign = np.where(np.arange(HEAD_DIM) < half, -1.0, 1.0)[None, :]
    inners = [np.cos(inner), np.sin(inner), np.cos(inner) * sign, np.sin(inner) * sign]
    return np.concatenate(inners + [np.cos(base), np.sin(base)]).astype(np.float32)


def doubling(order):
    held, steps = [0], []
    for mask in order:
        steps.append((mask, list(held)))
        held += [item ^ mask for item in held]
    return steps


def kernel(
    n, nx,
    order_hbm, q_hbm, k_hbm, v_hbm, cq_hbm, ck_hbm, cv_hbm, tables_hbm,
    out_v, cout_v,
    text, image, qs, tables, q_rot, gap, peak, total, mixed, order,
    load_sem, send_sem, text_recv, image_recv, mate_recv, ready,
):
    me = lax.axis_index("context")
    rows = qs.shape[1]
    span_len = rows // 2
    kv_local = text.shape[3] // HEAD_DIM
    image_rows = image.shape[3]
    paired = image.shape[1] == 2
    core = lax.axis_index("tensor") if paired else 0
    z, x = me // nx, me % nx

    x_masks = [1 << b for b in reversed(range(nx.bit_length() - 1))]
    z_masks = [nx << b for b in reversed(range((n // nx).bit_length() - 1))]
    masks = z_masks + x_masks
    z_x = doubling(z_masks + x_masks)
    z_x_z = doubling(z_masks[:1] + x_masks + z_masks[1:])
    x_z = doubling(x_masks + z_masks)
    part_steps = (z_x, z_x)
    image_steps = x_z

    def flipped(index, item):
        for mask in masks:
            bit = (item // mask) % 2
            index = index + mask * bit * (1 - 2 * ((index // mask) % 2))
        return index

    partner = {mask: flipped(me, mask) for mask in (range(1, n) if paired else masks)}

    barrier = pltpu.get_barrier_semaphore()

    def hail(sem, where):
        pl.semaphore_signal(sem, inc=1, device_id=where, device_id_type=pl.DeviceIdType.MESH)

    def greet():
        if not paired:
            for mask in masks:
                hail(barrier, {"context": partner[mask]})
            return
        hail(barrier, {"tensor": 1 - core})
        hail(barrier, {"context": partner[1]})
        hail(barrier, {"context": partner[2]})

        @pl.when(z == 0)
        def _():
            hail(barrier, {"context": me + 2 * nx})

        @pl.when(z == 1)
        def _():
            hail(barrier, {"context": me + nx})
            hail(barrier, {"context": me + 2 * nx})

        @pl.when(z == 2)
        def _():
            hail(barrier, {"context": me - nx})

    def meet():
        if not paired:
            pl.semaphore_wait(barrier, len(masks))
            return
        pl.semaphore_wait(barrier, 3 + jnp.where(z == 0, 0, jnp.where(z == 2, 2, 1)))

        @pl.when(z == 1)
        def _():
            hail(ready.at[0], {"context": me - nx})

        @pl.when(z == 2)
        def _():
            hail(ready.at[0], {"context": me - nx})
            hail(ready.at[0], {"context": me + nx})

        @pl.when(jnp.logical_and(z == 2, core == 0))
        def _():
            hail(ready.at[1], {"tensor": 1})

    greet()
    kv_loads = [
        pltpu.make_async_copy(k_hbm, text.at[0, 0], send_sem.at[0]),
        pltpu.make_async_copy(v_hbm, text.at[0, 1], send_sem.at[0]),
        pltpu.make_async_copy(ck_hbm, image.at[0, core, 0], send_sem.at[1]),
        pltpu.make_async_copy(cv_hbm, image.at[0, core, 1], send_sem.at[1]),
    ]
    other_loads = [
        pltpu.make_async_copy(order_hbm, order, load_sem.at[0]),
        pltpu.make_async_copy(tables_hbm, tables, load_sem.at[1]),
        pltpu.make_async_copy(q_hbm, qs.at[0], load_sem.at[2]),
        pltpu.make_async_copy(cq_hbm, qs.at[1], load_sem.at[2]),
    ]

    def landed(ref, sem):
        pltpu.make_async_copy(ref, ref, sem).wait()

    for load in kv_loads:
        load.start()
    for load in other_loads:
        load.start()
    landed(text.at[0], send_sem.at[0])
    landed(image.at[0, core], send_sem.at[1])
    meet()

    def text_sem(item, part):
        if not paired:
            return text_recv.at[item - 1, part]
        return text_recv.at[3, 0] if isinstance(item, int) and item == 1 else text_recv.at[item // 2 - 1, part]

    def image_sem(item):
        return image_recv.at[{1: 0, 4: 1, 5: 2}.get(item, 3) if paired else item - 1]

    def text_copy(item, part, mask):
        return pltpu.make_async_remote_copy(
            src_ref=text.at[item, part], dst_ref=text.at[item ^ mask, part],
            send_sem=send_sem.at[0], recv_sem=text_sem(item ^ mask, part),
            device_id={"context": partner[mask]}, device_id_type=pl.DeviceIdType.MESH)

    def image_copy(item, mask):
        return pltpu.make_async_remote_copy(
            src_ref=image.at[item], dst_ref=image.at[item ^ mask],
            send_sem=send_sem.at[1], recv_sem=image_sem(item ^ mask),
            device_id={"context": partner[mask]}, device_id_type=pl.DeviceIdType.MESH)

    def forward_text(item, part):
        for mask, held in part_steps[part]:
            if item in held:
                text_copy(item, part, mask).start()

    def forward_image(item):
        for mask, held in image_steps:
            if item in held:
                image_copy(item, mask).start()

    def arrive_text(item, part):
        text_copy(item ^ masks[0], part, masks[0]).wait_recv()
        forward_text(item, part)

    def arrive_image(item):
        image_copy(item ^ masks[0], masks[0]).wait_recv()
        forward_image(item)

    def send(kind, item, mask, cond=None, whole=None):
        if kind == 2 and (whole is False or whole is None and (item ^ mask) in DIRECT):
            copies = [straight(item, item ^ mask, half, partner[mask]) for half in range(2)]
        else:
            copies = [image_copy(item, mask) if kind == 2 else text_copy(item, kind, mask)]
        for copy in copies:
            if cond is None:
                copy.start()
            else:
                pl.when(cond)(copy.start)

    def straight(item, to, half, where):
        return pltpu.make_async_remote_copy(
            src_ref=image.at[item, half], dst_ref=image.at[to, half],
            send_sem=send_sem.at[1], recv_sem=image_sem(to),
            device_id={"context": where, "tensor": half}, device_id_type=pl.DeviceIdType.MESH)

    def pick(*values):
        result = values[-1]
        for at in range(len(values) - 2, -1, -1):
            result = jnp.where(z == at, values[at], result)
        return result

    def relayed(item, part, to, sem):
        return pltpu.make_async_remote_copy(
            src_ref=text.at[item, part], dst_ref=text.at[to, part], send_sem=send_sem.at[0], recv_sem=sem,
            device_id={"context": partner[1]}, device_id_type=pl.DeviceIdType.MESH)

    def relay(at):
        place, part = at // 2, at % 2
        item = places[place]
        if at == 3:
            item, part = jnp.where(z == 0, places[2], item), jnp.where(z == 0, 0, 1)
        if at == 4:
            item, part = jnp.where(z == 0, places[1], item), jnp.where(z == 0, 1, 0)
        relayed(item, part, item, text_sem(item, part)).wait_recv()
        relayed(item, part, item + 1, text_recv.at[4, part] if place else text_recv.at[3, 1]).start()
        if place < 2:
            send(at % 2, 4, 2, z == 2 * place)

    def both_in(item, column):
        landed(text.at[item], text_recv.at[3, column])

    def texts_in(part):
        landed(text.at[0], text_recv.at[4, part])

    def take(item):
        image_copy(item ^ 1, 1).wait_recv()

    def handed(item, where):
        return pltpu.make_async_remote_copy(
            src_ref=image.at[item, 0], dst_ref=image.at[item, 0],
            send_sem=send_sem.at[2], recv_sem=image_sem(item) if item else mate_recv.at[0],
            device_id={"tensor": where}, device_id_type=pl.DeviceIdType.MESH)

    def carry(items):
        for item in items:
            take(item)
            handed(item, 0).start()

    def forward(item):
        @pl.when(z % 2 == 0)
        def _():
            carry([item])
            send(2, item, 2)

        @pl.when(z % 2 == 1)
        def _():
            straight(item, item, 1, partner[1]).wait_recv()

    def on_core(which):
        return pl.when(core == which)

    if paired:
        places = [pick(4, 2, 6, 2), pick(6, 4, 4, 4), pick(2, 6, 2, 6)]
        for part in range(2):
            send(part, 0, 1)
            send(part, 0, 2, z != 3)
            send(part, 0, 6, z == 1)
            send(part, 0, 4, z == 2)
        on_core(0)(handed(0, 1).start)

        @pl.when(z != 2)
        def _():
            pl.semaphore_wait(ready.at[0], 1)

        for mask, cond in ((6, z == 3), (2, z == 3), (4, z != 2)):
            for part in range(2):
                send(part, 0, mask, cond)

        @on_core(1)
        def _():
            handed(0, 0).wait_recv()
            send(2, 0, 1)

            @pl.when(z == 2)
            def _():
                pl.semaphore_wait(ready.at[1], 1)
                hail(ready.at[1], {"context": me + nx})
    else:
        forward_text(0, 0)
        forward_text(0, 1)
        forward_image(0)

    other_loads[0].wait()
    other_loads[1].wait()
    landed(qs, load_sem.at[2])

    spans = order.shape[0]

    def angles(place):
        inners = [tables[at * span_len:(at + 1) * span_len, :] for at in range(4)]
        cosines, sines, starts = [], [], []
        for part in range(2):
            span = order[2 * place + part]
            base_cos = tables[pl.ds(4 * span_len + span, 1), :]
            base_sin = tables[pl.ds(4 * span_len + spans + span, 1), :]
            cosines.append(base_cos * inners[0] - base_sin * inners[1])
            sines.append(base_sin * inners[2] + base_cos * inners[3])
            starts.append(span * span_len)
        return jnp.concatenate(cosines, 0), jnp.concatenate(sines, 0), starts

    def rotate(values, cosine, sine):
        values = values.astype(jnp.float32)
        turned = pltpu.roll(values, HEAD_DIM // 2, 1)
        return (values * cosine + turned * sine).astype(jnp.bfloat16)

    own_cos, own_sin, own_starts = angles(me)
    lane = lax.broadcasted_iota(jnp.int32, gap.shape, 1)
    for g in range(1, GROUP):
        lane = jnp.where(lane >= rows, lane - rows, lane)
    own_places = jnp.where(lane < span_len, own_starts[0] + lane, own_starts[1] + lane - span_len)
    gap[...] = own_places - lax.broadcasted_iota(jnp.int32, gap.shape, 0)
    for head in range(kv_local * GROUP):
        q_rot[head // GROUP, pl.ds(head % GROUP * rows, rows), :] = rotate(
            qs[0, :, head * HEAD_DIM:(head + 1) * HEAD_DIM], own_cos, own_sin)

    def dot_nt(a, b):
        return lax.dot_general(a, b, (((1,), (1,)), ((), ())), preferred_element_type=jnp.float32)

    def join(pieces):
        return pieces[0] if len(pieces) == 1 else jnp.concatenate(pieces, 0)

    def mix(values, weights):
        return lax.dot_general(
            values, weights.astype(jnp.bfloat16), (((0,), (0,)), ((), ())), preferred_element_type=jnp.float32)

    def folded(weights):
        return jnp.sum(weights.reshape(-1, 8, weights.shape[1]), 0)

    heads = range(kv_local)
    head_columns = [slice(head * HEAD_DIM, (head + 1) * HEAD_DIM) for head in heads]

    def weigh(items, first=False):
        parts = [angles(flipped(me, item)) for item in items]
        cosine, sine = join([p[0] for p in parts]), join([p[1] for p in parts])
        starts = sum([p[2] for p in parts], [])
        keys = [rotate(join([text[item, 0, :, at] for item in items]), cosine, sine) for at in head_columns]
        scores = [dot_nt(keys[head], q_rot[head]) for head in heads]
        scores = [join([
            jnp.where(gap[...] >= starts[at], block_scores[at * span_len:(at + 1) * span_len], NEG_FILL)
            for at in range(len(starts))]) for block_scores in scores]
        top = [jnp.max(block_scores, 0, keepdims=True) for block_scores in scores]
        if not first:
            old = [peak[head] for head in heads]
            top = [jnp.maximum(top[head], old[head]) for head in heads]
        weights = [jnp.exp2((scores[head] - top[head]) * SCALE) for head in heads]
        summed = [folded(weights[head]) for head in heads]
        if first:
            return top, weights, summed, None
        factor = [jnp.exp2((old[head] - top[head]) * SCALE) for head in heads]
        return top, weights, [summed[head] + total[head] * factor[head] for head in heads], factor

    def add(items, weighed, last=False):
        top, weights, summed, factor = weighed
        values = [join([text[item, 1, :, at] for item in items]) for at in head_columns]
        product = [mix(values[head], weights[head]) for head in heads]
        if factor is not None:
            product = [product[head] + mixed[head] * factor[head] for head in heads]
        if last:
            store(out_v, product, summed)
            return
        for head in heads:
            peak[head] = top[head]
            total[head] = summed[head]
            mixed[head] = product[head]

    def block(items, first=False):
        add(items, weigh(items, first))

    def store(target, product, summed):
        result = [
            (product[head] * (1.0 / jnp.sum(summed[head], 0, keepdims=True))).astype(jnp.bfloat16).T for head in heads]
        for head in heads:
            for g in range(GROUP):
                at = head * GROUP + g
                target[:, at * HEAD_DIM:(at + 1) * HEAD_DIM] = result[head][g * rows:(g + 1) * rows]

    def cross_weigh():
        keys_all = image[:, core, 0].astype(jnp.float32).reshape(n * image_rows, -1).astype(jnp.bfloat16)
        values_all = image[:, core, 1].astype(jnp.float32).reshape(n * image_rows, -1).astype(jnp.bfloat16)
        queries = [
            jnp.concatenate(
                [qs[1, :, h * HEAD_DIM:(h + 1) * HEAD_DIM] for h in range(head * GROUP, (head + 1) * GROUP)], 0)
            for head in heads]
        scores = [dot_nt(keys_all[:, head_columns[head]], queries[head]) for head in heads]
        top = [jnp.max(scores[head], 0, keepdims=True) for head in heads]
        weights = [jnp.exp2((scores[head] - top[head]) * SCALE) for head in heads]
        return values_all, weights, [folded(weights[head]) for head in heads]

    def cross_add(weighed):
        values_all, weights, summed = weighed
        store(cout_v, [mix(values_all[:, head_columns[head]], weights[head]) for head in heads], summed)

    def image_start(item):
        send(2, item, 4, z % 2 == 0)
        send(2, item, 4, z == 3, whole=False)
        send(2, item, 2)
        send(2, item, 6, z == 1)

    block([0], first=True)
    if paired:
        both_in(1, 0)
        block([1])
        relay(0)
        relay(1)
        relay(2)
        relay(3)

        @pl.when(jnp.logical_and(core == 1, z == 3))
        def _():
            pl.semaphore_wait(ready.at[1], 1)
            send(2, 0, 6)
            take(1)
            send(2, 1, 6)


        @on_core(1)
        def _():
            image_start(0)

        relay(4)
        relay(5)

        @on_core(1)
        def _():
            pl.when(z != 3)(functools.partial(take, 1))
            handed(1, 0).start()
            image_start(1)

        block(places)

        @on_core(1)
        def _():
            for item in range(2):
                send(2, item, 4, z == 1, whole=False)

        rest = [place + 1 for place in places]

        def images_in():
            for item in (1, 4, 5):
                handed(item, 0).wait_recv()
            landed(image.at[pl.ds(0, len(DIRECT)), 0], image_sem(DIRECT[0]))

        @on_core(0)
        def _():
            both_in(rest[0], 1)
            block(rest[:1])

            @pl.when(z > 0)
            def _():
                images_in()
                cross_add(cross_weigh())

            texts_in(0)
            weighed = weigh(rest[1:])

            @pl.when(z == 0)
            def _():
                images_in()
                crossed = cross_weigh()
                texts_in(1)
                add(rest[1:], weighed, last=True)
                cross_add(crossed)

            @pl.when(z > 0)
            def _():
                texts_in(1)
                add(rest[1:], weighed, last=True)

        @on_core(1)
        def _():
            forward(4)
            both_in(rest[0], 1)
            for part in range(2):
                texts_in(part)
            add(rest, weigh(rest), last=True)
            forward(5)
            landed(image.at[pl.ds(0, len(DIRECT)), 1], image_sem(DIRECT[0]))
            cross_add(cross_weigh())

        @on_core(0)
        def _():
            handed(0, 1).wait_send()

        @on_core(1)
        def _():
            landed(image.at[pl.ds(0, n - 1)], send_sem.at[1])
            handed(1, 0).wait_send()

            @pl.when(z % 2 == 0)
            def _():
                landed(image.at[pl.ds(0, 2), 0], send_sem.at[2])
    else:
        for part in range(2):
            for mask, held in part_steps[part]:
                for item in held:
                    arrive_text(item ^ mask, part)
        for mask, held in image_steps:
            for item in held:
                arrive_image(item ^ mask)

        def step(item, unused):
            block([item])
            return 0

        lax.fori_loop(1, n, step, 0)
        store(out_v, [mixed[head] for head in heads], [total[head] for head in heads])
        cross_add(cross_weigh())
        landed(image.at[pl.ds(0, n - 1)], send_sem.at[1])
    landed(text.at[pl.ds(0, n - 1)], send_sem.at[0])


def flush(self_v, cross_v, self_hbm, cross_hbm, sems):
    copies = [
        pltpu.make_async_copy(self_v, self_hbm, sems.at[0]),
        pltpu.make_async_copy(cross_v, cross_hbm, sems.at[1]),
    ]
    for copy in copies:
        copy.start()
    for copy in copies:
        copy.wait()


def body(n, nx, cores, self_queries, self_keys, self_values, cross_queries, cross_keys, cross_values, span_order):
    rows, width = self_queries.shape
    kv_width = self_keys.shape[1]
    kv_local = kv_width // HEAD_DIM
    image_rows = cross_keys.shape[0]
    tables = rotary_tables(span_order.shape[0], rows // 2)
    anywhere = pl.BlockSpec(memory_space=pl.ANY)
    result = pltpu.VMEM((rows, width), jnp.bfloat16)
    held = pl.pallas_call(
        functools.partial(kernel, n, nx),
        out_shape=(result, result),
        in_specs=[anywhere] * 8,
        out_specs=(pl.BlockSpec(memory_space=pltpu.VMEM),) * 2,
        scratch_shapes=[
            pltpu.VMEM((n, 2, rows, kv_width), jnp.bfloat16),
            pltpu.VMEM((n, cores, 2, image_rows, kv_width), jnp.bfloat16),
            pltpu.VMEM((2, rows, width), jnp.bfloat16),
            pltpu.VMEM(tables.shape, jnp.float32),
            pltpu.VMEM((kv_local, GROUP * rows, HEAD_DIM), jnp.bfloat16),
            pltpu.VMEM((rows // 2, GROUP * rows), jnp.int32),
            pltpu.VMEM((kv_local, 1, GROUP * rows), jnp.float32),
            pltpu.VMEM((kv_local, 8, GROUP * rows), jnp.float32),
            pltpu.VMEM((kv_local, HEAD_DIM, GROUP * rows), jnp.float32),
            pltpu.SMEM(span_order.shape, jnp.int32),
            pltpu.SemaphoreType.DMA((3,)),
            pltpu.SemaphoreType.DMA((3,)),
            pltpu.SemaphoreType.DMA((5 if cores == 2 else n - 1, 2)),
            pltpu.SemaphoreType.DMA((4 if cores == 2 else n - 1,)),
            pltpu.SemaphoreType.DMA((1,)),
            pltpu.SemaphoreType.REGULAR((2,)),
        ],
        compiler_params=pltpu.CompilerParams(collective_id=0, has_side_effects=True),
    )(span_order, self_queries, self_keys, self_values, cross_queries, cross_keys, cross_values, tables)
    plain = jax.ShapeDtypeStruct((rows, width), jnp.bfloat16)
    return pl.pallas_call(
        flush,
        out_shape=(plain, plain),
        in_specs=[pl.BlockSpec(memory_space=pltpu.VMEM)] * 2,
        out_specs=(anywhere, anywhere),
        scratch_shapes=[pltpu.SemaphoreType.DMA((2,))],
    )(*[pltpu.with_memory_space_constraint(array, pltpu.VMEM) for array in held])


def fast_axis(mesh, n):
    line = mesh.devices[0, :, 0]
    coords = [getattr(device, "coords", None) for device in line]
    if any(c is None for c in coords):
        return 1
    nx = len({c[0] for c in coords})
    return nx if n % nx == 0 else 1


def solution(mesh):
    n = mesh.shape["context"]
    nx = fast_axis(mesh, n)
    cores = 2 if (n, nx, mesh.shape["tensor"]) == (8, 2, 2) else 1
    both = P(("groups", "context"), "tensor")
    return jax.shard_map(
        functools.partial(body, n, nx, cores), mesh=mesh,
        in_specs=(both,) * 6 + (P("groups"),), out_specs=(both, both), check_vma=False)
```
